32 devices in a mesh: dp: 8 (over z, y), mp: 4 (over x, core).
Axes of the slice: x: 2, y: 2, z: 4, core: 2. Of those that a mesh axis runs over, the one named last changes fastest.
Arguments:
- slow_weights: float32 [1, 3584, 1024], P(None, None, 'mp'), may hold values from -6 to 6
- fast_weights: bfloat16 [8, 1, 3584, 1024], P('dp', None, None, 'mp'), may hold values from -64 to 64
- momentum: float32 [1, 3584, 1024], P(None, None, 'mp'), may hold values from -1.2 to 1.2
Outputs:
- slow_next: float32 [1, 3584, 1024], P(None, None, 'mp')
- momentum_next: float32 [1, 3584, 1024], P(None, None, 'mp')
- fast_next: bfloat16 [8, 1, 3584, 1024], P('dp', None, None, 'mp')
The draws below stay inside these ranges and needn't reach their ends.
All inputs are finite; a program needn't handle non-finite values.
Results may differ from the reference program's by a relative error of at most 0.001.
Values sent between devices are 32-bit elements; how exact they have to be, the bound alone decides.
A program may use at most 64 MiB of HBM per device.

```python
import math
import jax
import jax.numpy as jnp
from jax import lax

D = 3584
LAYERS = 1
KV2 = 1024
REPLICAS = 8


def slow_base(key):
    values = jax.random.normal(jax.random.fold_in(key, 11), (LAYERS, D, KV2), jnp.float32)
    return jnp.clip(values, -6.0, 6.0)


def draw_slow_weights(key, part):
    return slow_base(key)


def draw_fast_weights(key, part):
    slow_values = slow_base(key)
    row_place = jnp.arange(D, dtype=jnp.float32) / D
    col_place = jnp.arange(KV2, dtype=jnp.float32) / KV2
    row_spread = 10.0 ** jax.random.uniform(jax.random.fold_in(key, 12), (D,), jnp.float32)
    col_spread = 10.0 ** jax.random.uniform(jax.random.fold_in(key, 13), (KV2,), jnp.float32)
    common = jax.random.normal(jax.random.fold_in(key, 14), (LAYERS, D, KV2), jnp.float32)
    single = jax.random.normal(jax.random.fold_in(key, 15), (REPLICAS, LAYERS, D, KV2), jnp.float32)
    row_scale = (1.0 + 2.0 * row_place) * row_spread
    col_scale = (1.0 + 2.0 * col_place) * col_spread
    drift = 0.02 * (common[None] + 1.5 * single)
    drift = drift * row_scale[:, None] * col_scale[None, :]
    fast_values = jnp.clip(slow_values[None] - drift, -64.0, 64.0)
    return fast_values.astype(jnp.bfloat16)


def shard_levels(rng, extent, cuts, least, high):
    factor_of = 1.0
    for axis_at, shards_of in cuts:
        heights = jax.random.uniform(jax.random.fold_in(jax.random.fold_in(rng, 6), axis_at), (shards_of,), jnp.float32, least / len(cuts), high / len(cuts))
        factor_of = factor_of * jnp.repeat(jnp.exp(heights), extent[axis_at] // shards_of).reshape((-1,) + (1,) * (len(extent) - 1 - axis_at))
    return factor_of


def gaussian(own_key, dims, deviation, reach, pieces=(), kind=jnp.bfloat16):
    result = jax.random.normal(own_key, dims, jnp.float32) * deviation
    if len(pieces) > 0:
        result = shard_levels(own_key, dims, pieces, -0.22, 0.18) * result
    return jnp.clip(result, min=-reach, max=reach).astype(kind)


def setup_inputs(seed: int = 0) -> dict:
    splits = jax.random.split(jax.random.key(seed), 4)
    return {
        "slow_weights": draw_slow_weights(jax.random.fold_in(splits[3], 71), 0),
        "fast_weights": draw_fast_weights(jax.random.fold_in(splits[3], 71), 0),
        "momentum": gaussian(splits[2], (LAYERS, D, KV2), 0.2, 1.2, ((2, 4),), jnp.float32),
    }


MOMENTUM_RATE = 0.9
OUTER_RATE = 0.7
CLIP_LEVEL = 0.2
EPSILON = 1e-06

def reference(slow_weights, fast_weights, momentum):

    def accumulate(summed, fast_one):
        return (summed + (slow_weights - fast_one.astype(jnp.float32)), None)
    summed, unused = lax.scan(accumulate, jnp.zeros_like(slow_weights), fast_weights)
    pseudo = summed / REPLICAS
    norm_value = jnp.sqrt(jnp.sum(pseudo * pseudo))
    max_norm = CLIP_LEVEL * math.sqrt(LAYERS * D * KV2)
    factor = jnp.minimum(1.0, max_norm / (norm_value + EPSILON))
    gradient = factor * pseudo
    momentum_next = MOMENTUM_RATE * momentum + gradient
    slow_next = slow_weights - OUTER_RATE * (gradient + MOMENTUM_RATE * momentum_next)
    fast_next = jnp.broadcast_to(slow_next.astype(jnp.bfloat16)[None], fast_weights.shape)
    return (slow_next, momentum_next, fast_next)
```

```python
import functools
import math

import jax
import jax.numpy as jnp
from jax import lax
from jax.experimental import pallas as pl
from jax.experimental.pallas import tpu as pltpu
from jax.sharding import PartitionSpec as P

MOMENTUM_RATE = 0.9
OUTER_RATE = 0.7
CLIP_LEVEL = 0.2
EPSILON = 1e-06
MESH = pl.DeviceIdType.MESH
SUBS = 4
VMEM_LIMIT = 24 * 1024 * 1024
LADDER_LIMIT = 40 * 1024 * 1024

OUTER = (
    (3, 0, 1, 0), (11, 0, 4, 0), (7, 0, 4, 0), (51, 0, 1, 0), (2, 0, 1, 0), (9, 0, 4, 0),
    (1, 0, 1, 0), (45, 0, 4, 0), (10, 4, 1, 0), (5, 1, 4, 0), (6, 4, 1, 0), (47, 1, 4, 0),
    (0, 0, 1, 0), (41, 1, 4, 0), (8, 4, 1, 0), (53, 1, 4, 0), (4, 4, 1, 0), (43, 0, 4, 0),
    (46, 4, 1, 0), (55, 0, 4, 0), (49, 0, 1, 0), (35, 1, 4, 0), (44, 4, 1, 0), (37, 1, 4, 0),
    (50, 0, 1, 0), (21, 1, 4, 0), (48, 0, 1, 0), (33, 0, 4, 0), (42, 4, 1, 0), (31, 0, 4, 0),
    (40, 4, 1, 0), (39, 0, 4, 0), (54, 4, 1, 0), (27, 1, 4, 0), (15, 0, 1, 0), (19, 0, 4, 0),
    (34, 4, 1, 0), (23, 1, 4, 0), (52, 4, 1, 0), (29, 0, 4, 0), (32, 4, 1, 0), (6, 8, 32, 2),
    (13, 0, 1, 0), (25, 0, 4, 0), (14, 0, 1, 0), (8, 8, 32, 2), (30, 4, 1, 0), (48, 8, 32, 2),
    (26, 4, 1, 0), (4, 8, 32, 2), (12, 0, 1, 0), (46, 8, 32, 2), (28, 4, 1, 0), (50, 8, 32, 2),
    (49, 8, 8, 2), (44, 8, 32, 2), (24, 4, 1, 0), (40, 8, 32, 2), (38, 4, 1, 0), (52, 8, 32, 2),
    (22, 4, 1, 0), (42, 8, 32, 2), (18, 4, 1, 0), (54, 8, 32, 2), (17, 0, 1, 0), (34, 8, 32, 2),
    (36, 4, 1, 0), (32, 8, 32, 2), (20, 4, 1, 0), (12, 8, 32, 2), (16, 0, 1, 0), (28, 8, 32, 2),
    (24, 8, 32, 2), (30, 8, 32, 2), (13, 8, 8, 2), (26, 8, 32, 2), (36, 8, 32, 2), (31, 8, 8, 2),
    (16, 8, 32, 2), (38, 8, 32, 2), (37, 8, 8, 2), (22, 8, 32, 2), (17, 8, 8, 2), (0, 8, 0, 2),
    (2, 8, 0, 2), (1, 8, 0, 2), (10, 8, 0, 2), (3, 8, 0, 2), (11, 8, 0, 2), (7, 8, 0, 2),
    (9, 8, 0, 2), (5, 8, 0, 2), (47, 8, 0, 2), (51, 8, 0, 2), (45, 8, 0, 2), (41, 8, 0, 2),
    (53, 8, 0, 2), (43, 8, 0, 2), (14, 8, 0, 2), (55, 8, 0, 2), (35, 8, 0, 2), (33, 8, 0, 2),
    (15, 8, 0, 2), (29, 8, 0, 2), (25, 8, 0, 2), (20, 8, 0, 2), (27, 8, 0, 2), (21, 8, 0, 2),
    (39, 8, 0, 2), (18, 8, 0, 2), (23, 8, 0, 2), (19, 8, 0, 2),
)
INNER = (
    (5, 0, 1, 0), (47, 0, 1, 0), (9, 0, 4, 0), (11, 0, 4, 0), (41, 0, 1, 0), (7, 0, 4, 0),
    (53, 0, 1, 0), (45, 0, 4, 0), (3, 1, 2, 0), (35, 0, 1, 0), (43, 0, 4, 0), (51, 1, 2, 0),
    (27, 0, 1, 0), (55, 0, 4, 0), (2, 1, 2, 0), (37, 0, 1, 0), (33, 0, 4, 0), (21, 0, 1, 0),
    (1, 3, 4, 0), (10, 5, 2, 0), (23, 0, 1, 0), (29, 0, 4, 0), (6, 5, 2, 0), (25, 0, 4, 0),
    (0, 3, 4, 0), (0, 4, 24, 3), (8, 7, 56, 1), (4, 3, 56, 1), (46, 1, 2, 0), (31, 0, 4, 0),
    (2, 8, 8, 2), (1, 4, 24, 3), (49, 3, 4, 0), (10, 8, 40, 2), (50, 1, 2, 0), (6, 8, 40, 2),
    (44, 7, 56, 1), (3, 8, 8, 2), (42, 5, 2, 0), (39, 0, 4, 0), (48, 7, 24, 1), (19, 0, 4, 0),
    (11, 8, 8, 2), (54, 5, 2, 0), (46, 8, 40, 2), (15, 1, 2, 0), (50, 8, 40, 2), (34, 1, 2, 0),
    (40, 3, 56, 1), (52, 3, 56, 1), (32, 7, 56, 1), (13, 3, 4, 0), (14, 1, 2, 0), (42, 8, 40, 2),
    (30, 5, 2, 0), (54, 8, 40, 2), (26, 1, 2, 0), (34, 8, 40, 2), (12, 7, 24, 1), (28, 7, 56, 1),
    (14, 8, 40, 2), (24, 7, 56, 1), (30, 8, 8, 2), (38, 5, 2, 0), (22, 1, 2, 0), (15, 8, 8, 2),
    (26, 8, 40, 2), (18, 5, 2, 0), (17, 1, 4, 0), (36, 3, 24, 1), (20, 3, 56, 1), (16, 7, 24, 1),
    (-1, 0, 0, 4), (38, 8, 40, 2), (22, 8, 40, 2), (21, 8, 8, 2), (-1, 0, 0, 5), (18, 8, 40, 2),
    (19, 8, 8, 2), (9, 8, 0, 2), (5, 8, 0, 2), (7, 8, 0, 2), (45, 8, 0, 2), (47, 8, 0, 2),
    (51, 8, 0, 2), (41, 8, 0, 2), (53, 8, 0, 2), (33, 8, 0, 2), (43, 8, 0, 2), (49, 8, 0, 2),
    (55, 8, 0, 2), (35, 8, 0, 2), (29, 8, 0, 2), (25, 8, 0, 2), (27, 8, 0, 2), (13, 8, 0, 2),
    (39, 8, 0, 2), (23, 8, 0, 2), (31, 8, 0, 2), (37, 8, 0, 2), (17, 8, 0, 2),
)


def ladder_kernel(n, m, max_norm, slow_hbm, fast_hbm, moment_hbm,
                  pseudo, slow_ref, moment_ref, factor_ref,
                  fast_ref, part, inbox, square, norms, parts,
                  moment_sem, load_sem, send_sem, recv_sem, norm_send, norm_recv, part_send, part_recv):
    rows, cols = slow_ref.shape
    groups = load_sem.shape[1]
    size = rows // (4 * groups)
    half = n // 4
    me = lax.axis_index("dp")
    mine = lax.axis_index("mp")
    z, y = me // 2, lax.rem(me, 2)
    upper = z // half
    step = 1 - 2 * upper
    outer = lax.rem(z + upper, half) == 0
    away = jnp.where(outer, step, -step)
    near = 2 * (z + away) + y
    across = 2 * (z + step) + y
    rung = 2 * z + 1 - y
    target = (near, across, rung)
    spots = [(far + upper - 2 * far * upper) * 2 + (other + y - 2 * other * y) for far in range(2) for other in range(2)]
    block = size * 4

    def load(g):
        at = pl.ds(g * block, block)
        return (
            pltpu.make_async_copy(slow_hbm.at[at], slow_ref.at[at], load_sem.at[0, g]),
            pltpu.make_async_copy(fast_hbm.at[at], fast_ref.at[at], load_sem.at[1, g]),
        )

    loads = []
    for entry in OUTER + INNER:
        if entry[0] >= 0 and entry[0] // 4 not in loads:
            loads.append(entry[0] // 4)
    for g in loads[:2]:
        for copy in load(g):
            copy.start()
    barrier = pltpu.get_barrier_semaphore()
    for other in (near, rung):
        pl.semaphore_signal(barrier, inc=1, device_id={"dp": other}, device_id_type=MESH)
    for k in range(1, m):
        pl.semaphore_signal(
            barrier, inc=1, device_id={"mp": lax.rem(mine + k, m)}, device_id_type=MESH
        )

    @pl.when(jnp.logical_not(outer))
    def _():
        pl.semaphore_signal(barrier, inc=1, device_id={"dp": across}, device_id_type=MESH)

    for g in loads[2:]:
        for copy in load(g):
            copy.start()
    moment_load = pltpu.make_async_copy(moment_hbm, moment_ref, moment_sem)
    moment_load.start()
    square[...] = jnp.zeros_like(square)

    def place(chunk):
        return (chunk // 4) * 4 + spots[chunk % 4]

    def at_of(spot):
        return pl.ds(pl.multiple_of(spot * size, size), size)

    def sum_copy(spot, k):
        at = at_of(spot)
        return pltpu.make_async_remote_copy(
            src_ref=part.at[at], dst_ref=inbox.at[k, at], send_sem=send_sem, recv_sem=recv_sem.at[k, spot],
            device_id={"dp": target[k]}, device_id_type=MESH,
        )

    def mean_copy(spot, k):
        at = at_of(spot)
        return pltpu.make_async_remote_copy(
            src_ref=pseudo.at[at], dst_ref=pseudo.at[at], send_sem=send_sem, recv_sem=recv_sem.at[3, spot],
            device_id={"dp": target[k]}, device_id_type=MESH,
        )

    def norm_copy(k):
        return pltpu.make_async_remote_copy(
            src_ref=norms.at[mine], dst_ref=norms.at[mine], send_sem=norm_send.at[k], recv_sem=norm_recv.at[k],
            device_id={"mp": lax.rem(mine + k, m)}, device_id_type=MESH,
        )

    def part_copy(k):
        return pltpu.make_async_remote_copy(
            src_ref=parts.at[me], dst_ref=parts.at[me], send_sem=part_send.at[k], recv_sem=part_recv.at[me],
            device_id={"dp": lax.rem(me + k, n)}, device_id_type=MESH,
        )

    roots = [2 * q + c for q in (half - 1, half) for c in range(2)]

    def part_wait(j):
        pltpu.make_async_remote_copy(
            src_ref=parts.at[j], dst_ref=parts.at[j], send_sem=part_send.at[0], recv_sem=part_recv.at[j],
            device_id={"dp": lax.rem(me + 1, n)}, device_id_type=MESH,
        ).wait_recv()

    def run(steps):
        seen = set()
        sent = 0
        for chunk, waits, sends, kind in steps:
            if kind == 4:
                norms[mine] = square[:, : cols // 2] + square[:, cols // 2 :]
                for k in range(1, m):
                    norm_copy(k).start()
                continue
            if kind == 5:
                for k in range(1, m):
                    norm_copy(k).wait_recv()
                total = norms[0]
                for j in range(1, m):
                    total = total + norms[j]
                parts[me] = total
                for k in range(1, n):
                    part_copy(k).start()
                continue
            g = chunk // 4
            if kind != 2 and g not in seen:
                seen.add(g)
                for copy in load(g):
                    copy.wait()
            spot = place(chunk)
            at = at_of(spot)
            for k in range(3):
                if waits >> k & 1:
                    sum_copy(spot, k).wait_recv()
            if waits & 8:
                mean_copy(spot, 2).wait_recv()
            if kind in (0, 1, 3):
                value = part[at] if kind == 3 else slow_ref[at] - fast_ref[at].astype(jnp.float32)
                for k in range(3):
                    if waits >> k & 1:
                        value = value + inbox[k, at]
                if kind == 0:
                    part[at] = value
                else:
                    value = value * (1.0 / n)
                    pseudo[at] = value
            for k in (1, 0, 2):
                if sends >> k & 1:
                    sum_copy(spot, k).start()
                    sent += 1
                if sends >> (3 + k) & 1:
                    mean_copy(spot, k).start()
                    sent += 1
            if kind in (1, 3):
                weight = 1.0 if kind == 1 else 0.5
                square[...] += weight * jnp.sum((value * value).reshape(size // 8, 8, cols), axis=0)
        for g in loads:
            if g not in seen:
                for copy in load(g):
                    copy.wait()
        whole = inbox.reshape(3 * rows, cols).at[pl.ds(0, sent * size)]
        pltpu.make_async_copy(whole, whole, send_sem).wait()

    @pl.when(outer)
    def _():
        pl.semaphore_wait(barrier, m + 1)
        run(OUTER)
        for j in roots:
            part_wait(j)

    @pl.when(jnp.logical_not(outer))
    def _():
        pl.semaphore_wait(barrier, m + 2)
        run(INNER)
        for k in range(1, m):
            norm_copy(k).wait_send()
        for k in range(1, n):
            part_copy(k).wait_send()
        for j in roots:

            @pl.when(me != j)
            def _():
                part_wait(j)

    total = parts[roots[0]]
    for j in roots[1:]:
        total = total + parts[j]
    total = jnp.sum(jnp.sum(total, axis=1, keepdims=True), axis=0, keepdims=True)
    factor = jnp.minimum(1.0, max_norm / (jnp.sqrt(total) + EPSILON))
    factor_ref[...] = jnp.broadcast_to(factor, factor_ref.shape)
    moment_load.wait()


def update_kernel(pieces, pseudo, slow_ref, moment_ref, factor_ref,
                  slow_out, moment_out, fast_out, slow_new, moment_new, fast_new, sem):
    rows, cols = slow_ref.shape
    size = rows // pieces
    factor = factor_ref[0:1, 0:1]

    def copies(k):
        at = pl.ds(pl.multiple_of(k * size, size), size)
        pairs = ((slow_new, slow_out), (moment_new, moment_out), (fast_new, fast_out))
        return [pltpu.make_async_copy(a.at[at], b.at[at], sem.at[i, k]) for i, (a, b) in enumerate(pairs)]

    def piece(k, carry):
        at = pl.ds(pl.multiple_of(k * size, size), size)
        gradient = factor * pseudo[at]
        moment = MOMENTUM_RATE * moment_ref[at] + gradient
        slow = slow_ref[at] - OUTER_RATE * (gradient + MOMENTUM_RATE * moment)
        moment_new[at] = moment
        slow_new[at] = slow
        fast_new[at] = slow.astype(fast_new.dtype)
        for copy in copies(k):
            copy.start()
        return carry

    def finish(k, carry):
        for copy in copies(k):
            copy.wait()
        return carry

    lax.fori_loop(0, pieces, piece, 0)
    lax.fori_loop(0, pieces, finish, 0)


def ladder(n, m, max_norm, slow, fast, moment):
    rows, cols = slow.shape
    groups = 1 + max(e[0] for e in OUTER + INNER) // 4
    hbm = pl.BlockSpec(memory_space=pltpu.HBM)
    vmem = pl.BlockSpec(memory_space=pltpu.VMEM)
    whole = jax.ShapeDtypeStruct((rows, cols), jnp.float32)
    dma = pltpu.SemaphoreType.DMA
    flat = [pltpu.with_memory_space_constraint(x, pltpu.HBM) for x in (slow, fast, moment)]
    results = pl.pallas_call(
        functools.partial(ladder_kernel, n, m, max_norm),
        out_shape=(whole, whole, whole, jax.ShapeDtypeStruct((8, 128), jnp.float32)),
        in_specs=[hbm, hbm, hbm],
        out_specs=(vmem, vmem, vmem, vmem),
        scratch_shapes=[
            pltpu.VMEM((rows, cols), fast.dtype),
            pltpu.VMEM((rows, cols), jnp.float32),
            pltpu.VMEM((3, rows, cols), jnp.float32),
            pltpu.VMEM((8, cols), jnp.float32),
            pltpu.VMEM((m, 8, cols // 2), jnp.float32),
            pltpu.VMEM((n, 8, cols // 2), jnp.float32),
            dma,
            dma((2, groups)),
            dma,
            dma((4, 4 * groups)),
            dma((m,)),
            dma((m,)),
            dma((n,)),
            dma((n,)),
        ],
        compiler_params=pltpu.CompilerParams(
            collective_id=0, has_side_effects=True, vmem_limit_bytes=LADDER_LIMIT
        ),
        name="ladder",
    )(*flat)
    pieces = 14
    while rows % (pieces * 16):
        pieces -= 1
    return pl.pallas_call(
        functools.partial(update_kernel, pieces),
        out_shape=(whole, whole, jax.ShapeDtypeStruct((rows, cols), fast.dtype)),
        in_specs=[vmem] * 4,
        out_specs=(hbm, hbm, hbm),
        scratch_shapes=[
            pltpu.VMEM((rows, cols), jnp.float32),
            pltpu.VMEM((rows, cols), jnp.float32),
            pltpu.VMEM((rows, cols), fast.dtype),
            dma((3, pieces)),
        ],
        compiler_params=pltpu.CompilerParams(vmem_limit_bytes=VMEM_LIMIT),
        name="update",
    )(*results)


def device_at(place, n):
    half = n // 2
    up = 2 * place
    down = 2 * (n - 1 - place) + 1
    return jnp.where(place < half, up, down)


def ring_kernel(n, m, subs, max_norm, slow_hbm, fast_hbm, moment_hbm,
           slow_out, moment_out, fast_out,
           ring, slow_ref, fast_ref, moment_ref, pseudo_ref, parts, norms, moment_sem, load_sem, send_sem, recv_sem,
           part_send, part_recv, norm_send, norm_recv):
    rows, cols = slow_ref.shape
    chunk = rows // n
    sub = chunk // subs
    half = cols // 2
    me = lax.axis_index("dp")
    mine = lax.axis_index("mp")
    z, y = me // 2, lax.rem(me, 2)
    place = jnp.where(y == 0, z, n - 1 - z)
    right = device_at(lax.rem(place + 1, n), n)
    left = device_at(lax.rem(place + n - 1, n), n)
    goal = (right, left)
    order = (place, lax.rem(n - place, n))

    def load(d, k):
        c = lax.rem(order[d] - k + n, n)
        at = (pl.ds(pl.multiple_of(c * chunk, chunk), chunk), pl.ds(d * half, half))
        return (
            pltpu.make_async_copy(slow_hbm.at[at], slow_ref.at[at], load_sem.at[0, d, k]),
            pltpu.make_async_copy(fast_hbm.at[at], fast_ref.at[at], load_sem.at[1, d, k]),
        )

    for d in range(2):
        for copy in load(d, 0):
            copy.start()
    barrier = pltpu.get_barrier_semaphore()
    for other in (left, right):
        pl.semaphore_signal(barrier, inc=1, device_id={"dp": other}, device_id_type=MESH)
    for k in range(1, m):
        pl.semaphore_signal(
            barrier, inc=1, device_id={"mp": lax.rem(mine + k, m)}, device_id_type=MESH
        )
    moment_load = pltpu.make_async_copy(moment_hbm, moment_ref, moment_sem)

    def start_row(c, b):
        return pl.multiple_of(c * chunk + b * sub, sub)

    def own(d, b, c):
        at = (pl.ds(start_row(c, b), sub), pl.ds(d * half, half))
        return slow_ref[at] - fast_ref[at].astype(jnp.float32)

    def reduce_copy(d, b, s):
        return pltpu.make_async_remote_copy(
            src_ref=ring.at[d, b, s], dst_ref=ring.at[d, b, s + 1],
            send_sem=send_sem.at[d, b, s], recv_sem=recv_sem.at[d, b, s],
            device_id={"dp": goal[d]}, device_id_type=MESH,
        )

    def gather_copy(d, b, s, c):
        at = (pl.ds(start_row(c, b), sub), pl.ds(d * half, half))
        return pltpu.make_async_remote_copy(
            src_ref=pseudo_ref.at[at], dst_ref=pseudo_ref.at[at],
            send_sem=send_sem.at[d, b, n - 1 + s], recv_sem=recv_sem.at[d, b, n - 1 + s],
            device_id={"dp": goal[d]}, device_id_type=MESH,
        )

    def part_copy(k):
        return pltpu.make_async_remote_copy(
            src_ref=parts.at[me], dst_ref=parts.at[me],
            send_sem=part_send.at[k], recv_sem=part_recv.at[k],
            device_id={"dp": lax.rem(me + k, n)}, device_id_type=MESH,
        )

    def norm_copy(k):
        return pltpu.make_async_remote_copy(
            src_ref=norms.at[mine], dst_ref=norms.at[mine],
            send_sem=norm_send.at[k], recv_sem=norm_recv.at[k],
            device_id={"mp": lax.rem(mine + k, m)}, device_id_type=MESH,
        )

    streams = [(d, b) for b in range(subs) for d in range(2)]
    for k in range(1, n):
        for d in range(2):
            for copy in load(d, k):
                copy.start()
    for d in range(2):
        for copy in load(d, 0):
            copy.wait()
    pl.semaphore_wait(barrier, 2 + m - 1)
    for d, b in streams:
        ring[d, b, 0] = own(d, b, order[d])
        reduce_copy(d, b, 0).start()
    moment_load.start()

    def reduce_step(s, carry):
        for d in range(2):
            for copy in load(d, s + 1):
                copy.wait()
        for d, b in streams:
            c = lax.rem(order[d] - s - 1 + n, n)
            reduce_copy(d, b, s).wait_recv()
            ring[d, b, s + 1] = ring[d, b, s + 1] + own(d, b, c)
            reduce_copy(d, b, s + 1).start()
        return carry

    lax.fori_loop(0, n - 2, reduce_step, 0)
    for d in range(2):
        for copy in load(d, n - 1):
            copy.wait()
    part = jnp.zeros((8, half), jnp.float32)
    for d, b in streams:
        c = lax.rem(order[d] + 1, n)
        reduce_copy(d, b, n - 2).wait_recv()
        value = (ring[d, b, n - 1] + own(d, b, c)) / n
        pseudo_ref[pl.ds(start_row(c, b), sub), pl.ds(d * half, half)] = value
        gather_copy(d, b, 0, c).start()
        part = part + jnp.sum((value * value).reshape(sub // 8, 8, half), axis=0)
    parts[me] = part

    def gather_step(s, carry):
        for d, b in streams:
            c = lax.rem(order[d] - s + n, n)
            gather_copy(d, b, s, c).wait_recv()
            gather_copy(d, b, s + 1, c).start()
        return carry

    second = (n - 2) // 2
    first = second // 2
    for k in range(1, n):
        part_copy(k).start()
    lax.fori_loop(0, first, gather_step, 0)
    for k in range(1, n):
        part_copy(k).wait_recv()
    norm = parts[0]
    for j in range(1, n):
        norm = norm + parts[j]
    norms[mine] = norm
    for k in range(1, m):
        norm_copy(k).start()
    lax.fori_loop(first, second, gather_step, 0)
    for k in range(1, m):
        norm_copy(k).wait_recv()
    total = norms[0]
    for j in range(1, m):
        total = total + norms[j]
    total = jnp.sum(jnp.sum(total, axis=1, keepdims=True), axis=0, keepdims=True)
    factor = jnp.minimum(1.0, max_norm / (jnp.sqrt(total) + EPSILON))
    moment_load.wait()

    def update(d, c, start=0, size=chunk):
        at = (pl.ds(pl.multiple_of(c * chunk + start, 16), size), pl.ds(d * half, half))
        gradient = factor * pseudo_ref[at]
        moment = MOMENTUM_RATE * moment_ref[at] + gradient
        slow = slow_ref[at] - OUTER_RATE * (gradient + MOMENTUM_RATE * moment)
        moment_out[at] = moment
        slow_out[at] = slow
        fast_out[at] = slow.astype(fast_out.dtype)

    def update_step(s, carry):
        gather_step(s, carry)
        for d in range(2):
            update(d, lax.rem(order[d] - s + n, n))
            update(d, lax.rem(order[d] - (s - second) + n, n))
        return carry

    lax.fori_loop(second, n - 2, update_step, 0)
    for d in range(2):
        update(d, lax.rem(order[d] + 1, n))
    for k in range(1, n):
        part_copy(k).wait_send()
    for k in range(1, m):
        norm_copy(k).wait_send()

    def drain(s, carry):
        for d, b in streams:
            reduce_copy(d, b, s).wait_send()
            gather_copy(d, b, s, 0).wait_send()
        return carry

    lax.fori_loop(0, n - 2, drain, 0)
    for d, b in streams:
        c = lax.rem(order[d] + 2, n)
        reduce_copy(d, b, n - 2).wait_send()
        gather_copy(d, b, n - 2, c).wait()
        update(d, c, b * sub, sub)


def emit_kernel(pieces, *refs):
    count = len(refs) // 2
    sources, targets, sem = refs[:count], refs[count:-1], refs[-1]
    size = sources[0].shape[0] // pieces
    copies = [
        pltpu.make_async_copy(
            sources[i].at[pl.ds(k * size, size)], targets[i].at[pl.ds(k * size, size)], sem.at[i, k]
        )
        for k in range(pieces) for i in range(count)
    ]
    for copy in copies:
        copy.start()
    for copy in copies:
        copy.wait()


def emit(arrays, pieces):
    return pl.pallas_call(
        functools.partial(emit_kernel, pieces),
        out_shape=tuple(jax.ShapeDtypeStruct(x.shape, x.dtype) for x in arrays),
        in_specs=[pl.BlockSpec(memory_space=pltpu.VMEM)] * len(arrays),
        out_specs=tuple(pl.BlockSpec(memory_space=pltpu.HBM) for _ in arrays),
        scratch_shapes=[pltpu.SemaphoreType.DMA((len(arrays), pieces))],
        compiler_params=pltpu.CompilerParams(vmem_limit_bytes=VMEM_LIMIT),
        name="emit",
    )(*arrays)


def ring(n, m, max_norm, slow, fast, moment):
    rows, cols = slow.shape
    subs = SUBS
    while rows % (n * subs * 16):
        subs -= 1
    sub = rows // (n * subs)
    hbm = pl.BlockSpec(memory_space=pltpu.HBM)
    vmem = pl.BlockSpec(memory_space=pltpu.VMEM)
    flat = [pltpu.with_memory_space_constraint(x, pltpu.HBM) for x in (slow, fast, moment)]
    results = pl.pallas_call(
        functools.partial(ring_kernel, n, m, subs, max_norm),
        out_shape=(
            jax.ShapeDtypeStruct((rows, cols), jnp.float32),
            jax.ShapeDtypeStruct((rows, cols), jnp.float32),
            jax.ShapeDtypeStruct((rows, cols), jnp.bfloat16),
        ),
        in_specs=[hbm, hbm, hbm],
        out_specs=(vmem, vmem, vmem),
        scratch_shapes=[
            pltpu.VMEM((2, subs, n, sub, cols // 2), jnp.float32),
            pltpu.VMEM((rows, cols), jnp.float32),
            pltpu.VMEM((rows, cols), jnp.bfloat16),
            pltpu.VMEM((rows, cols), jnp.float32),
            pltpu.VMEM((rows, cols), jnp.float32),
            pltpu.VMEM((n, 8, cols // 2), jnp.float32),
            pltpu.VMEM((m, 8, cols // 2), jnp.float32),
            pltpu.SemaphoreType.DMA,
            pltpu.SemaphoreType.DMA((2, 2, n)),
            pltpu.SemaphoreType.DMA((2, subs, 2 * n - 2)),
            pltpu.SemaphoreType.DMA((2, subs, 2 * n - 2)),
            pltpu.SemaphoreType.DMA((n,)),
            pltpu.SemaphoreType.DMA((n,)),
            pltpu.SemaphoreType.DMA((m,)),
            pltpu.SemaphoreType.DMA((m,)),
        ],
        compiler_params=pltpu.CompilerParams(
            collective_id=0, has_side_effects=True, vmem_limit_bytes=VMEM_LIMIT
        ),
        name="ring",
    )(*flat)
    return emit(results, 4)


def body(slow_weights, fast_weights, momentum):
    n, m = lax.axis_size("dp"), lax.axis_size("mp")
    layers, depth, cols = slow_weights.shape
    rows = layers * depth
    max_norm = CLIP_LEVEL * math.sqrt(rows * cols * m)
    flat = [x.reshape(rows, cols) for x in (slow_weights, fast_weights, momentum)]
    groups = 1 + max(e[0] for e in OUTER + INNER) // 4
    columns = n // 2
    form = ladder if columns == 4 and rows % (groups * 4 * 16) == 0 else ring
    slow_next, momentum_next, fast_next = form(n, m, max_norm, *flat)
    return (
        slow_next.reshape(slow_weights.shape),
        momentum_next.reshape(slow_weights.shape),
        fast_next.reshape(fast_weights.shape),
    )


def solution(mesh):
    in_specs = (P(None, None, "mp"), P("dp", None, None, "mp"), P(None, None, "mp"))
    out_specs = (P(None, None, "mp"), P(None, None, "mp"), P("dp", None, None, "mp"))
    return jax.shard_map(body, mesh=mesh, in_specs=in_specs, out_specs=out_specs, check_vma=False)
```

```python
import functools
import math

import jax
import jax.numpy as jnp
from jax import lax
from jax.experimental import pallas as pl
from jax.experimental.pallas import tpu as pltpu
from jax.sharding import PartitionSpec as P

MOMENTUM_RATE = 0.9
OUTER_RATE = 0.7
CLIP_LEVEL = 0.2
EPSILON = 1e-06
MESH = pl.DeviceIdType.MESH
SUBS = 4
VMEM_LIMIT = 24 * 1024 * 1024
LADDER_LIMIT = 40 * 1024 * 1024

SIZES = (3, 7, 7, 7, 6, 3, 2, 4, 1, 7, 2, 7)
OUTER = (
    (35, 0, 4, 0), (23, 0, 1, 0), (31, 0, 4, 0), (22, 0, 1, 0), (29, 0, 4, 0), (21, 0, 1, 0),
    (33, 0, 4, 0), (43, 0, 1, 0), (11, 0, 4, 0), (34, 4, 1, 0), (20, 0, 1, 0), (30, 4, 1, 0),
    (9, 0, 4, 0), (28, 4, 1, 0), (42, 0, 1, 0), (15, 0, 4, 0), (41, 0, 1, 0), (10, 4, 1, 0),
    (13, 0, 4, 0), (40, 0, 1, 0), (27, 0, 1, 0), (3, 1, 4, 0), (26, 0, 1, 0), (14, 4, 1, 0),
    (39, 0, 4, 0), (47, 0, 1, 0), (1, 1, 4, 0), (25, 0, 4, 0), (37, 1, 4, 0), (2, 4, 1, 0),
    (38, 4, 1, 0), (19, 0, 4, 0), (46, 0, 1, 0), (7, 1, 4, 0), (5, 0, 1, 0), (17, 0, 4, 0),
    (18, 4, 1, 0), (45, 0, 4, 0), (6, 4, 1, 0), (32, 5, 40, 1), (8, 5, 40, 1), (12, 5, 40, 1),
    (0, 5, 40, 1), (24, 5, 40, 1), (36, 5, 40, 1), (44, 5, 40, 1), (16, 5, 40, 1), (34, 8, 32, 2),
    (4, 1, 40, 1), (-1, 0, 0, 4), (10, 8, 32, 2), (35, 8, 8, 2), (-1, 0, 0, 5), (14, 8, 32, 2),
    (5, 8, 8, 2), (2, 8, 32, 2), (11, 8, 8, 2), (26, 8, 32, 2), (38, 8, 32, 2), (15, 8, 8, 2),
    (3, 8, 8, 2), (46, 8, 32, 2), (27, 8, 8, 2), (18, 8, 32, 2), (20, 8, 0, 2), (21, 8, 0, 2),
    (28, 8, 0, 2), (22, 8, 0, 2), (23, 8, 0, 2), (30, 8, 0, 2), (29, 8, 0, 2), (40, 8, 0, 2),
    (31, 8, 0, 2), (41, 8, 0, 2), (42, 8, 0, 2), (33, 8, 0, 2), (9, 8, 0, 2), (43, 8, 0, 2),
    (13, 8, 0, 2), (1, 8, 0, 2), (25, 8, 0, 2), (37, 8, 0, 2), (45, 8, 0, 2), (17, 8, 0, 2),
    (39, 8, 0, 2), (6, 8, 0, 2), (47, 8, 0, 2), (19, 8, 0, 2), (7, 8, 0, 2),
)
INNER = (
    (35, 0, 4, 0), (31, 0, 4, 0), (3, 0, 1, 0), (7, 0, 1, 0), (33, 0, 4, 0), (11, 0, 4, 0),
    (1, 0, 1, 0), (23, 1, 2, 0), (29, 0, 4, 0), (37, 0, 1, 0), (22, 1, 2, 0), (15, 0, 4, 0),
    (43, 1, 2, 0), (34, 5, 2, 0), (21, 3, 4, 0), (20, 3, 4, 0), (30, 5, 2, 0), (32, 6, 1, 0),
    (9, 0, 4, 0), (42, 1, 2, 0), (20, 4, 24, 3), (39, 0, 4, 0), (21, 4, 24, 3), (28, 7, 56, 1),
    (10, 5, 2, 0), (22, 8, 8, 2), (40, 3, 4, 0), (23, 8, 8, 2), (41, 3, 4, 0), (27, 1, 4, 0),
    (30, 8, 8, 2), (13, 0, 4, 0), (14, 5, 2, 0), (29, 8, 24, 2), (19, 0, 4, 0), (8, 6, 1, 0),
    (26, 5, 2, 0), (47, 1, 4, 0), (2, 1, 2, 0), (40, 4, 24, 3), (12, 6, 1, 0), (25, 0, 4, 0),
    (38, 5, 2, 0), (45, 0, 4, 0), (31, 8, 8, 2), (41, 4, 24, 3), (-1, 0, 0, 4), (17, 0, 4, 0),
    (42, 8, 8, 2), (46, 5, 2, 0), (0, 2, 1, 0), (36, 2, 1, 0), (-1, 0, 0, 5), (5, 1, 4, 0),
    (18, 5, 2, 0), (43, 8, 8, 2), (24, 6, 1, 0), (44, 6, 1, 0), (6, 1, 2, 0), (32, 8, 48, 2),
    (16, 6, 1, 0), (8, 8, 48, 2), (4, 6, 1, 0), (12, 8, 48, 2), (34, 8, 8, 2), (0, 8, 48, 2),
    (10, 8, 8, 2), (24, 8, 48, 2), (36, 8, 48, 2), (14, 8, 8, 2), (2, 8, 8, 2), (44, 8, 48, 2),
    (26, 8, 8, 2), (16, 8, 48, 2), (38, 8, 40, 2), (4, 8, 16, 2), (46, 8, 40, 2), (18, 8, 40, 2),
    (5, 8, 16, 2), (6, 8, 8, 2), (7, 8, 8, 2), (33, 8, 0, 2), (9, 8, 0, 2), (13, 8, 0, 2),
    (1, 8, 0, 2), (25, 8, 0, 2), (37, 8, 0, 2), (45, 8, 0, 2), (35, 8, 0, 2), (17, 8, 0, 2),
    (39, 8, 0, 2), (11, 8, 0, 2), (47, 8, 0, 2), (15, 8, 0, 2), (19, 8, 0, 2), (3, 8, 0, 2),
    (27, 8, 0, 2),
)

def ladder_kernel(n, m, max_norm, slow_hbm, fast_hbm, moment_hbm,
                  pseudo, slow_ref, moment_ref, factor_ref,
                  fast_ref, part, inbox, square, norms, parts,
                  moment_sem, load_sem, send_sem, recv_sem, norm_send, norm_recv, part_send, part_recv):
    rows, cols = slow_ref.shape
    groups = load_sem.shape[1]
    unit = rows // (4 * sum(SIZES))
    sizes = [unit * s for s in SIZES]
    bases = [4 * sum(sizes[:g]) for g in range(groups)]
    half = n // 4
    me = lax.axis_index("dp")
    mine = lax.axis_index("mp")
    z, y = me // 2, lax.rem(me, 2)
    upper = z // half
    step = 1 - 2 * upper
    outer = lax.rem(z + upper, half) == 0
    away = jnp.where(outer, step, -step)
    near = 2 * (z + away) + y
    across = 2 * (z + step) + y
    rung = 2 * z + 1 - y
    target = (near, across, rung)
    spots = [(far + upper - 2 * far * upper) * 2 + (other + y - 2 * other * y) for far in range(2) for other in range(2)]

    def load(g):
        at = pl.ds(bases[g], 4 * sizes[g])
        return (
            pltpu.make_async_copy(slow_hbm.at[at], slow_ref.at[at], load_sem.at[0, g]),
            pltpu.make_async_copy(fast_hbm.at[at], fast_ref.at[at], load_sem.at[1, g]),
        )

    loads = []
    for entry in OUTER + INNER:
        if entry[0] >= 0 and entry[0] // 4 not in loads:
            loads.append(entry[0] // 4)
    for g in loads[:2]:
        for copy in load(g):
            copy.start()
    barrier = pltpu.get_barrier_semaphore()
    for other in (near, rung):
        pl.semaphore_signal(barrier, inc=1, device_id={"dp": other}, device_id_type=MESH)
    for k in range(1, m):
        pl.semaphore_signal(
            barrier, inc=1, device_id={"mp": lax.rem(mine + k, m)}, device_id_type=MESH
        )

    @pl.when(jnp.logical_not(outer))
    def _():
        pl.semaphore_signal(barrier, inc=1, device_id={"dp": across}, device_id_type=MESH)

    for g in loads[2:]:
        for copy in load(g):
            copy.start()
    moment_load = pltpu.make_async_copy(moment_hbm, moment_ref, moment_sem)
    moment_load.start()
    square[...] = jnp.zeros_like(square)

    def at_of(chunk):
        g = chunk // 4
        return pl.ds(pl.multiple_of(bases[g] + spots[chunk % 4] * sizes[g], 16), sizes[g])

    def sum_copy(chunk, k):
        at = at_of(chunk)
        return pltpu.make_async_remote_copy(
            src_ref=part.at[at], dst_ref=inbox.at[k, at], send_sem=send_sem,
            recv_sem=recv_sem.at[k, chunk // 4 * 4 + spots[chunk % 4]],
            device_id={"dp": target[k]}, device_id_type=MESH,
        )

    def mean_copy(chunk, k):
        at = at_of(chunk)
        return pltpu.make_async_remote_copy(
            src_ref=pseudo.at[at], dst_ref=pseudo.at[at], send_sem=send_sem,
            recv_sem=recv_sem.at[3, chunk // 4 * 4 + spots[chunk % 4]],
            device_id={"dp": target[k]}, device_id_type=MESH,
        )

    def norm_copy(k):
        return pltpu.make_async_remote_copy(
            src_ref=norms.at[mine], dst_ref=norms.at[mine], send_sem=norm_send.at[k], recv_sem=norm_recv.at[k],
            device_id={"mp": lax.rem(mine + k, m)}, device_id_type=MESH,
        )

    def part_copy(k):
        return pltpu.make_async_remote_copy(
            src_ref=parts.at[me], dst_ref=parts.at[me], send_sem=part_send.at[k], recv_sem=part_recv.at[k],
            device_id={"dp": lax.rem(me + k, n)}, device_id_type=MESH,
        )

    def run(steps):
        seen = set()
        sent = 0
        for chunk, waits, sends, kind in steps:
            if kind == 4:
                norms[mine] = square[:, : cols // 2] + square[:, cols // 2 :]
                for k in range(1, m):
                    norm_copy(k).start()
                continue
            if kind == 5:
                for k in range(1, m):
                    norm_copy(k).wait_recv()
                total = norms[0]
                for j in range(1, m):
                    total = total + norms[j]
                parts[me] = total
                for k in range(1, n):
                    part_copy(k).start()
                continue
            g = chunk // 4
            if kind != 2 and g not in seen:
                seen.add(g)
                for copy in load(g):
                    copy.wait()
            at = at_of(chunk)
            for k in range(3):
                if waits >> k & 1:
                    sum_copy(chunk, k).wait_recv()
            if waits & 8:
                mean_copy(chunk, 2).wait_recv()
            if kind in (0, 1, 3):
                value = part[at] if kind == 3 else slow_ref[at] - fast_ref[at].astype(jnp.float32)
                for k in range(3):
                    if waits >> k & 1:
                        value = value + inbox[k, at]
                if kind == 0:
                    part[at] = value
                else:
                    value = value * (1.0 / n)
                    pseudo[at] = value
            for k in (1, 0, 2):
                if sends >> k & 1:
                    sum_copy(chunk, k).start()
                    sent += sizes[g]
                if sends >> (3 + k) & 1:
                    mean_copy(chunk, k).start()
                    sent += sizes[g]
            if kind in (1, 3):
                weight = 1.0 if kind == 1 else 0.5
                square[...] += weight * jnp.sum((value * value).reshape(sizes[g] // 8, 8, cols), axis=0)
        for g in loads:
            if g not in seen:
                for copy in load(g):
                    copy.wait()
        whole = inbox.reshape(3 * rows, cols).at[pl.ds(0, sent)]
        pltpu.make_async_copy(whole, whole, send_sem).wait()

    @pl.when(outer)
    def _():
        pl.semaphore_wait(barrier, m + 1)
        run(OUTER)

    @pl.when(jnp.logical_not(outer))
    def _():
        pl.semaphore_wait(barrier, m + 2)
        run(INNER)

    for k in range(1, m):
        norm_copy(k).wait_send()
    for k in range(1, n):
        part_copy(k).wait()
    total = parts[0]
    for j in range(1, n):
        total = total + parts[j]
    total = jnp.sum(jnp.sum(total, axis=1, keepdims=True), axis=0, keepdims=True)
    factor = jnp.minimum(1.0, max_norm / (jnp.sqrt(total) + EPSILON))
    factor_ref[...] = jnp.broadcast_to(factor, factor_ref.shape)
    moment_load.wait()


def update_kernel(pieces, pseudo, slow_ref, moment_ref, factor_ref,
                  slow_out, moment_out, fast_out, slow_new, moment_new, fast_new, sem):
    rows, cols = slow_ref.shape
    size = rows // pieces
    factor = factor_ref[0:1, 0:1]

    def copies(k):
        at = pl.ds(pl.multiple_of(k * size, size), size)
        pairs = ((slow_new, slow_out), (moment_new, moment_out), (fast_new, fast_out))
        return [pltpu.make_async_copy(a.at[at], b.at[at], sem.at[i, k]) for i, (a, b) in enumerate(pairs)]

    def piece(k, carry):
        at = pl.ds(pl.multiple_of(k * size, size), size)
        gradient = factor * pseudo[at]
        moment = MOMENTUM_RATE * moment_ref[at] + gradient
        slow = slow_ref[at] - OUTER_RATE * (gradient + MOMENTUM_RATE * moment)
        moment_new[at] = moment
        slow_new[at] = slow
        fast_new[at] = slow.astype(fast_new.dtype)
        for copy in copies(k):
            copy.start()
        return carry

    def finish(k, carry):
        for copy in copies(k):
            copy.wait()
        return carry

    lax.fori_loop(0, pieces, piece, 0)
    lax.fori_loop(0, pieces, finish, 0)


def ladder(n, m, max_norm, slow, fast, moment):
    rows, cols = slow.shape
    groups = len(SIZES)
    hbm = pl.BlockSpec(memory_space=pltpu.HBM)
    vmem = pl.BlockSpec(memory_space=pltpu.VMEM)
    whole = jax.ShapeDtypeStruct((rows, cols), jnp.float32)
    dma = pltpu.SemaphoreType.DMA
    flat = [pltpu.with_memory_space_constraint(x, pltpu.HBM) for x in (slow, fast, moment)]
    results = pl.pallas_call(
        functools.partial(ladder_kernel, n, m, max_norm),
        out_shape=(whole, whole, whole, jax.ShapeDtypeStruct((8, 128), jnp.float32)),
        in_specs=[hbm, hbm, hbm],
        out_specs=(vmem, vmem, vmem, vmem),
        scratch_shapes=[
            pltpu.VMEM((rows, cols), fast.dtype),
            pltpu.VMEM((rows, cols), jnp.float32),
            pltpu.VMEM((3, rows, cols), jnp.float32),
            pltpu.VMEM((8, cols), jnp.float32),
            pltpu.VMEM((m, 8, cols // 2), jnp.float32),
            pltpu.VMEM((n, 8, cols // 2), jnp.float32),
            dma,
            dma((2, groups)),
            dma,
            dma((4, 4 * groups)),
            dma((m,)),
            dma((m,)),
            dma((n,)),
            dma((n,)),
        ],
        compiler_params=pltpu.CompilerParams(
            collective_id=0, has_side_effects=True, vmem_limit_bytes=LADDER_LIMIT
        ),
        name="ladder",
    )(*flat)
    pieces = 14
    while rows % (pieces * 16):
        pieces -= 1
    return pl.pallas_call(
        functools.partial(update_kernel, pieces),
        out_shape=(whole, whole, jax.ShapeDtypeStruct((rows, cols), fast.dtype)),
        in_specs=[vmem] * 4,
        out_specs=(hbm, hbm, hbm),
        scratch_shapes=[
            pltpu.VMEM((rows, cols), jnp.float32),
            pltpu.VMEM((rows, cols), jnp.float32),
            pltpu.VMEM((rows, cols), fast.dtype),
            dma((3, pieces)),
        ],
        compiler_params=pltpu.CompilerParams(vmem_limit_bytes=VMEM_LIMIT),
        name="update",
    )(*results)


def device_at(place, n):
    half = n // 2
    up = 2 * place
    down = 2 * (n - 1 - place) + 1
    return jnp.where(place < half, up, down)


def ring_kernel(n, m, subs, max_norm, slow_hbm, fast_hbm, moment_hbm,
           slow_out, moment_out, fast_out,
           ring, slow_ref, fast_ref, moment_ref, pseudo_ref, parts, norms, moment_sem, load_sem, send_sem, recv_sem,
           part_send, part_recv, norm_send, norm_recv):
    rows, cols = slow_ref.shape
    chunk = rows // n
    sub = chunk // subs
    half = cols // 2
    me = lax.axis_index("dp")
    mine = lax.axis_index("mp")
    z, y = me // 2, lax.rem(me, 2)
    place = jnp.where(y == 0, z, n - 1 - z)
    right = device_at(lax.rem(place + 1, n), n)
    left = device_at(lax.rem(place + n - 1, n), n)
    goal = (right, left)
    order = (place, lax.rem(n - place, n))

    def load(d, k):
        c = lax.rem(order[d] - k + n, n)
        at = (pl.ds(pl.multiple_of(c * chunk, chunk), chunk), pl.ds(d * half, half))
        return (
            pltpu.make_async_copy(slow_hbm.at[at], slow_ref.at[at], load_sem.at[0, d, k]),
            pltpu.make_async_copy(fast_hbm.at[at], fast_ref.at[at], load_sem.at[1, d, k]),
        )

    for d in range(2):
        for copy in load(d, 0):
            copy.start()
    barrier = pltpu.get_barrier_semaphore()
    for other in (left, right):
        pl.semaphore_signal(barrier, inc=1, device_id={"dp": other}, device_id_type=MESH)
    for k in range(1, m):
        pl.semaphore_signal(
            barrier, inc=1, device_id={"mp": lax.rem(mine + k, m)}, device_id_type=MESH
        )
    moment_load = pltpu.make_async_copy(moment_hbm, moment_ref, moment_sem)

    def start_row(c, b):
        return pl.multiple_of(c * chunk + b * sub, sub)

    def own(d, b, c):
        at = (pl.ds(start_row(c, b), sub), pl.ds(d * half, half))
        return slow_ref[at] - fast_ref[at].astype(jnp.float32)

    def reduce_copy(d, b, s):
        return pltpu.make_async_remote_copy(
            src_ref=ring.at[d, b, s], dst_ref=ring.at[d, b, s + 1],
            send_sem=send_sem.at[d, b, s], recv_sem=recv_sem.at[d, b, s],
            device_id={"dp": goal[d]}, device_id_type=MESH,
        )

    def gather_copy(d, b, s, c):
        at = (pl.ds(start_row(c, b), sub), pl.ds(d * half, half))
        return pltpu.make_async_remote_copy(
            src_ref=pseudo_ref.at[at], dst_ref=pseudo_ref.at[at],
            send_sem=send_sem.at[d, b, n - 1 + s], recv_sem=recv_sem.at[d, b, n - 1 + s],
            device_id={"dp": goal[d]}, device_id_type=MESH,
        )

    def part_copy(k):
        return pltpu.make_async_remote_copy(
            src_ref=parts.at[me], dst_ref=parts.at[me],
            send_sem=part_send.at[k], recv_sem=part_recv.at[k],
            device_id={"dp": lax.rem(me + k, n)}, device_id_type=MESH,
        )

    def norm_copy(k):
        return pltpu.make_async_remote_copy(
            src_ref=norms.at[mine], dst_ref=norms.at[mine],
            send_sem=norm_send.at[k], recv_sem=norm_recv.at[k],
            device_id={"mp": lax.rem(mine + k, m)}, device_id_type=MESH,
        )

    streams = [(d, b) for b in range(subs) for d in range(2)]
    for k in range(1, n):
        for d in range(2):
            for copy in load(d, k):
                copy.start()
    for d in range(2):
        for copy in load(d, 0):
            copy.wait()
    pl.semaphore_wait(barrier, 2 + m - 1)
    for d, b in streams:
        ring[d, b, 0] = own(d, b, order[d])
        reduce_copy(d, b, 0).start()
    moment_load.start()

    def reduce_step(s, carry):
        for d in range(2):
            for copy in load(d, s + 1):
                copy.wait()
        for d, b in streams:
            c = lax.rem(order[d] - s - 1 + n, n)
            reduce_copy(d, b, s).wait_recv()
            ring[d, b, s + 1] = ring[d, b, s + 1] + own(d, b, c)
            reduce_copy(d, b, s + 1).start()
        return carry

    lax.fori_loop(0, n - 2, reduce_step, 0)
    for d in range(2):
        for copy in load(d, n - 1):
            copy.wait()
    part = jnp.zeros((8, half), jnp.float32)
    for d, b in streams:
        c = lax.rem(order[d] + 1, n)
        reduce_copy(d, b, n - 2).wait_recv()
        value = (ring[d, b, n - 1] + own(d, b, c)) / n
        pseudo_ref[pl.ds(start_row(c, b), sub), pl.ds(d * half, half)] = value
        gather_copy(d, b, 0, c).start()
        part = part + jnp.sum((value * value).reshape(sub // 8, 8, half), axis=0)
    parts[me] = part

    def gather_step(s, carry):
        for d, b in streams:
            c = lax.rem(order[d] - s + n, n)
            gather_copy(d, b, s, c).wait_recv()
            gather_copy(d, b, s + 1, c).start()
        return carry

    second = (n - 2) // 2
    first = second // 2
    for k in range(1, n):
        part_copy(k).start()
    lax.fori_loop(0, first, gather_step, 0)
    for k in range(1, n):
        part_copy(k).wait_recv()
    norm = parts[0]
    for j in range(1, n):
        norm = norm + parts[j]
    norms[mine] = norm
    for k in range(1, m):
        norm_copy(k).start()
    lax.fori_loop(first, second, gather_step, 0)
    for k in range(1, m):
        norm_copy(k).wait_recv()
    total = norms[0]
    for j in range(1, m):
        total = total + norms[j]
    total = jnp.sum(jnp.sum(total, axis=1, keepdims=True), axis=0, keepdims=True)
    factor = jnp.minimum(1.0, max_norm / (jnp.sqrt(total) + EPSILON))
    moment_load.wait()

    def update(d, c, start=0, size=chunk):
        at = (pl.ds(pl.multiple_of(c * chunk + start, 16), size), pl.ds(d * half, half))
        gradient = factor * pseudo_ref[at]
        moment = MOMENTUM_RATE * moment_ref[at] + gradient
        slow = slow_ref[at] - OUTER_RATE * (gradient + MOMENTUM_RATE * moment)
        moment_out[at] = moment
        slow_out[at] = slow
        fast_out[at] = slow.astype(fast_out.dtype)

    def update_step(s, carry):
        gather_step(s, carry)
        for d in range(2):
            update(d, lax.rem(order[d] - s + n, n))
            update(d, lax.rem(order[d] - (s - second) + n, n))
        return carry

    lax.fori_loop(second, n - 2, update_step, 0)
    for d in range(2):
        update(d, lax.rem(order[d] + 1, n))
    for k in range(1, n):
        part_copy(k).wait_send()
    for k in range(1, m):
        norm_copy(k).wait_send()

    def drain(s, carry):
        for d, b in streams:
            reduce_copy(d, b, s).wait_send()
            gather_copy(d, b, s, 0).wait_send()
        return carry

    lax.fori_loop(0, n - 2, drain, 0)
    for d, b in streams:
        c = lax.rem(order[d] + 2, n)
        reduce_copy(d, b, n - 2).wait_send()
        gather_copy(d, b, n - 2, c).wait()
        update(d, c, b * sub, sub)


def emit_kernel(pieces, *refs):
    count = len(refs) // 2
    sources, targets, sem = refs[:count], refs[count:-1], refs[-1]
    size = sources[0].shape[0] // pieces
    copies = [
        pltpu.make_async_copy(
            sources[i].at[pl.ds(k * size, size)], targets[i].at[pl.ds(k * size, size)], sem.at[i, k]
        )
        for k in range(pieces) for i in range(count)
    ]
    for copy in copies:
        copy.start()
    for copy in copies:
        copy.wait()


def emit(arrays, pieces):
    return pl.pallas_call(
        functools.partial(emit_kernel, pieces),
        out_shape=tuple(jax.ShapeDtypeStruct(x.shape, x.dtype) for x in arrays),
        in_specs=[pl.BlockSpec(memory_space=pltpu.VMEM)] * len(arrays),
        out_specs=tuple(pl.BlockSpec(memory_space=pltpu.HBM) for _ in arrays),
        scratch_shapes=[pltpu.SemaphoreType.DMA((len(arrays), pieces))],
        compiler_params=pltpu.CompilerParams(vmem_limit_bytes=VMEM_LIMIT),
        name="emit",
    )(*arrays)


def ring(n, m, max_norm, slow, fast, moment):
    rows, cols = slow.shape
    subs = SUBS
    while rows % (n * subs * 16):
        subs -= 1
    sub = rows // (n * subs)
    hbm = pl.BlockSpec(memory_space=pltpu.HBM)
    vmem = pl.BlockSpec(memory_space=pltpu.VMEM)
    flat = [pltpu.with_memory_space_constraint(x, pltpu.HBM) for x in (slow, fast, moment)]
    results = pl.pallas_call(
        functools.partial(ring_kernel, n, m, subs, max_norm),
        out_shape=(
            jax.ShapeDtypeStruct((rows, cols), jnp.float32),
            jax.ShapeDtypeStruct((rows, cols), jnp.float32),
            jax.ShapeDtypeStruct((rows, cols), jnp.bfloat16),
        ),
        in_specs=[hbm, hbm, hbm],
        out_specs=(vmem, vmem, vmem),
        scratch_shapes=[
            pltpu.VMEM((2, subs, n, sub, cols // 2), jnp.float32),
            pltpu.VMEM((rows, cols), jnp.float32),
            pltpu.VMEM((rows, cols), jnp.bfloat16),
            pltpu.VMEM((rows, cols), jnp.float32),
            pltpu.VMEM((rows, cols), jnp.float32),
            pltpu.VMEM((n, 8, cols // 2), jnp.float32),
            pltpu.VMEM((m, 8, cols // 2), jnp.float32),
            pltpu.SemaphoreType.DMA,
            pltpu.SemaphoreType.DMA((2, 2, n)),
            pltpu.SemaphoreType.DMA((2, subs, 2 * n - 2)),
            pltpu.SemaphoreType.DMA((2, subs, 2 * n - 2)),
            pltpu.SemaphoreType.DMA((n,)),
            pltpu.SemaphoreType.DMA((n,)),
            pltpu.SemaphoreType.DMA((m,)),
            pltpu.SemaphoreType.DMA((m,)),
        ],
        compiler_params=pltpu.CompilerParams(
            collective_id=0, has_side_effects=True, vmem_limit_bytes=VMEM_LIMIT
        ),
        name="ring",
    )(*flat)
    return emit(results, 4)


def body(slow_weights, fast_weights, momentum):
    n, m = lax.axis_size("dp"), lax.axis_size("mp")
    layers, depth, cols = slow_weights.shape
    rows = layers * depth
    max_norm = CLIP_LEVEL * math.sqrt(rows * cols * m)
    flat = [x.reshape(rows, cols) for x in (slow_weights, fast_weights, momentum)]
    columns = n // 2
    form = ladder if columns == 4 and rows % (sum(SIZES) * 4 * 16) == 0 else ring
    slow_next, momentum_next, fast_next = form(n, m, max_norm, *flat)
    return (
        slow_next.reshape(slow_weights.shape),
        momentum_next.reshape(slow_weights.shape),
        fast_next.reshape(fast_weights.shape),
    )


def solution(mesh):
    in_specs = (P(None, None, "mp"), P("dp", None, None, "mp"), P(None, None, "mp"))
    out_specs = (P(None, None, "mp"), P(None, None, "mp"), P("dp", None, None, "mp"))
    return jax.shard_map(body, mesh=mesh, in_specs=in_specs, out_specs=out_specs, check_vma=False)
```

```python
import functools
import math

import jax
import jax.numpy as jnp
from jax import lax
from jax.experimental import pallas as pl
from jax.experimental.pallas import tpu as pltpu
from jax.sharding import PartitionSpec as P

MOMENTUM_RATE = 0.9
OUTER_RATE = 0.7
CLIP_LEVEL = 0.2
EPSILON = 1e-06
MESH = pl.DeviceIdType.MESH
SUBS = 4
VMEM_LIMIT = 24 * 1024 * 1024
LADDER_LIMIT = 40 * 1024 * 1024

SIZES = (3, 7, 7, 7, 6, 3, 2, 4, 1, 7, 2, 7)
OUTER = (
    (35, 0, 4, 0), (23, 0, 1, 0), (31, 0, 4, 0), (22, 0, 1, 0), (29, 0, 4, 0), (21, 0, 1, 0),
    (33, 0, 4, 0), (43, 0, 1, 0), (11, 0, 4, 0), (34, 4, 1, 0), (20, 0, 1, 0), (30, 4, 1, 0),
    (9, 0, 4, 0), (28, 4, 1, 0), (42, 0, 1, 0), (15, 0, 4, 0), (41, 0, 1, 0), (10, 4, 1, 0),
    (13, 0, 4, 0), (40, 0, 1, 0), (27, 0, 1, 0), (3, 1, 4, 0), (26, 0, 1, 0), (14, 4, 1, 0),
    (39, 0, 4, 0), (47, 0, 1, 0), (1, 1, 4, 0), (25, 0, 4, 0), (37, 1, 4, 0), (2, 4, 1, 0),
    (38, 4, 1, 0), (19, 0, 4, 0), (46, 0, 1, 0), (7, 1, 4, 0), (5, 0, 1, 0), (17, 0, 4, 0),
    (18, 4, 1, 0), (45, 0, 4, 0), (6, 4, 1, 0), (32, 5, 40, 1), (8, 5, 40, 1), (12, 5, 40, 1),
    (0, 5, 40, 1), (24, 5, 40, 1), (36, 5, 40, 1), (44, 5, 40, 1), (16, 5, 40, 1), (34, 8, 32, 2),
    (4, 1, 40, 1), (-1, 0, 0, 4), (10, 8, 32, 2), (35, 8, 8, 2), (-1, 0, 0, 5), (14, 8, 32, 2),
    (5, 8, 8, 2), (2, 8, 32, 2), (11, 8, 8, 2), (26, 8, 32, 2), (38, 8, 32, 2), (15, 8, 8, 2),
    (3, 8, 8, 2), (46, 8, 32, 2), (27, 8, 8, 2), (18, 8, 32, 2), (20, 8, 0, 2), (21, 8, 0, 2),
    (28, 8, 0, 2), (22, 8, 0, 2), (23, 8, 0, 2), (30, 8, 0, 2), (29, 8, 0, 2), (40, 8, 0, 2),
    (31, 8, 0, 2), (41, 8, 0, 2), (42, 8, 0, 2), (33, 8, 0, 2), (9, 8, 0, 2), (43, 8, 0, 2),
    (13, 8, 0, 2), (1, 8, 0, 2), (25, 8, 0, 2), (37, 8, 0, 2), (45, 8, 0, 2), (17, 8, 0, 2),
    (39, 8, 0, 2), (6, 8, 0, 2), (47, 8, 0, 2), (19, 8, 0, 2), (7, 8, 0, 2),
)
INNER = (
    (35, 0, 4, 0), (31, 0, 4, 0), (3, 0, 1, 0), (7, 0, 1, 0), (33, 0, 4, 0), (11, 0, 4, 0),
    (1, 0, 1, 0), (23, 1, 2, 0), (29, 0, 4, 0), (37, 0, 1, 0), (22, 1, 2, 0), (15, 0, 4, 0),
    (43, 1, 2, 0), (34, 5, 2, 0), (21, 3, 4, 0), (20, 3, 4, 0), (30, 5, 2, 0), (32, 6, 1, 0),
    (9, 0, 4, 0), (42, 1, 2, 0), (20, 4, 24, 3), (39, 0, 4, 0), (21, 4, 24, 3), (28, 7, 56, 1),
    (10, 5, 2, 0), (22, 8, 8, 2), (40, 3, 4, 0), (23, 8, 8, 2), (41, 3, 4, 0), (27, 1, 4, 0),
    (30, 8, 8, 2), (13, 0, 4, 0), (14, 5, 2, 0), (29, 8, 24, 2), (19, 0, 4, 0), (8, 6, 1, 0),
    (26, 5, 2, 0), (47, 1, 4, 0), (2, 1, 2, 0), (40, 4, 24, 3), (12, 6, 1, 0), (25, 0, 4, 0),
    (38, 5, 2, 0), (45, 0, 4, 0), (31, 8, 8, 2), (41, 4, 24, 3), (-1, 0, 0, 4), (17, 0, 4, 0),
    (42, 8, 8, 2), (46, 5, 2, 0), (0, 2, 1, 0), (36, 2, 1, 0), (-1, 0, 0, 5), (5, 1, 4, 0),
    (18, 5, 2, 0), (43, 8, 8, 2), (24, 6, 1, 0), (44, 6, 1, 0), (6, 1, 2, 0), (32, 8, 48, 2),
    (16, 6, 1, 0), (8, 8, 48, 2), (4, 6, 1, 0), (12, 8, 48, 2), (34, 8, 8, 2), (0, 8, 48, 2),
    (10, 8, 8, 2), (24, 8, 48, 2), (36, 8, 48, 2), (14, 8, 8, 2), (2, 8, 8, 2), (44, 8, 48, 2),
    (26, 8, 8, 2), (16, 8, 48, 2), (38, 8, 40, 2), (4, 8, 16, 2), (46, 8, 40, 2), (18, 8, 40, 2),
    (5, 8, 16, 2), (6, 8, 8, 2), (7, 8, 8, 2), (33, 8, 0, 2), (9, 8, 0, 2), (13, 8, 0, 2),
    (1, 8, 0, 2), (25, 8, 0, 2), (37, 8, 0, 2), (45, 8, 0, 2), (35, 8, 0, 2), (17, 8, 0, 2),
    (39, 8, 0, 2), (11, 8, 0, 2), (47, 8, 0, 2), (15, 8, 0, 2), (19, 8, 0, 2), (3, 8, 0, 2),
    (27, 8, 0, 2),
)

def ladder_kernel(n, m, max_norm, slow_hbm, fast_hbm, moment_hbm,
                  slow_new, moment_new, fast_new,
                  pseudo, slow_ref, moment_ref, fast_ref, part, inbox, square, norms, parts,
                  moment_sem, load_sem, send_sem, recv_sem, norm_send, norm_recv, part_send, part_recv):
    rows, cols = slow_ref.shape
    groups = load_sem.shape[1]
    unit = rows // (4 * sum(SIZES))
    sizes = [unit * s for s in SIZES]
    bases = [4 * sum(sizes[:g]) for g in range(groups)]
    half = n // 4
    me = lax.axis_index("dp")
    mine = lax.axis_index("mp")
    z, y = me // 2, lax.rem(me, 2)
    upper = z // half
    step = 1 - 2 * upper
    outer = lax.rem(z + upper, half) == 0
    away = jnp.where(outer, step, -step)
    near = 2 * (z + away) + y
    across = 2 * (z + step) + y
    rung = 2 * z + 1 - y
    target = (near, across, rung)
    spots = [(far + upper - 2 * far * upper) * 2 + (other + y - 2 * other * y) for far in range(2) for other in range(2)]

    def load(g):
        at = pl.ds(bases[g], 4 * sizes[g])
        return (
            pltpu.make_async_copy(slow_hbm.at[at], slow_ref.at[at], load_sem.at[0, g]),
            pltpu.make_async_copy(fast_hbm.at[at], fast_ref.at[at], load_sem.at[1, g]),
        )

    loads = []
    for entry in OUTER + INNER:
        if entry[0] >= 0 and entry[0] // 4 not in loads:
            loads.append(entry[0] // 4)
    for g in loads[:2]:
        for copy in load(g):
            copy.start()
    barrier = pltpu.get_barrier_semaphore()
    for other in (near, rung):
        pl.semaphore_signal(barrier, inc=1, device_id={"dp": other}, device_id_type=MESH)
    for k in range(1, m):
        pl.semaphore_signal(
            barrier, inc=1, device_id={"mp": lax.rem(mine + k, m)}, device_id_type=MESH
        )

    @pl.when(jnp.logical_not(outer))
    def _():
        pl.semaphore_signal(barrier, inc=1, device_id={"dp": across}, device_id_type=MESH)

    for g in loads[2:]:
        for copy in load(g):
            copy.start()
    moment_load = pltpu.make_async_copy(moment_hbm, moment_ref, moment_sem)
    moment_load.start()
    square[...] = jnp.zeros_like(square)

    def at_of(chunk):
        g = chunk // 4
        return pl.ds(pl.multiple_of(bases[g] + spots[chunk % 4] * sizes[g], 16), sizes[g])

    def sum_copy(chunk, k):
        at = at_of(chunk)
        return pltpu.make_async_remote_copy(
            src_ref=part.at[at], dst_ref=inbox.at[k, at], send_sem=send_sem,
            recv_sem=recv_sem.at[k, chunk // 4 * 4 + spots[chunk % 4]],
            device_id={"dp": target[k]}, device_id_type=MESH,
        )

    def mean_copy(chunk, k):
        at = at_of(chunk)
        return pltpu.make_async_remote_copy(
            src_ref=pseudo.at[at], dst_ref=pseudo.at[at], send_sem=send_sem,
            recv_sem=recv_sem.at[3, chunk // 4 * 4 + spots[chunk % 4]],
            device_id={"dp": target[k]}, device_id_type=MESH,
        )

    def norm_copy(k):
        return pltpu.make_async_remote_copy(
            src_ref=norms.at[mine], dst_ref=norms.at[mine], send_sem=norm_send.at[k], recv_sem=norm_recv.at[k],
            device_id={"mp": lax.rem(mine + k, m)}, device_id_type=MESH,
        )

    def part_copy(k):
        return pltpu.make_async_remote_copy(
            src_ref=parts.at[me], dst_ref=parts.at[me], send_sem=part_send.at[k], recv_sem=part_recv.at[k],
            device_id={"dp": lax.rem(me + k, n)}, device_id_type=MESH,
        )

    def clip():
        for k in range(1, n):
            part_copy(k).wait_recv()
        total = parts[0]
        for j in range(1, n):
            total = total + parts[j]
        total = jnp.sum(jnp.sum(total, axis=1, keepdims=True), axis=0, keepdims=True)
        moment_load.wait()
        return jnp.minimum(1.0, max_norm / (jnp.sqrt(total) + EPSILON))

    def update(factor, chunk):
        at = at_of(chunk)
        gradient = factor * pseudo[at]
        moment = MOMENTUM_RATE * moment_ref[at] + gradient
        slow = slow_ref[at] - OUTER_RATE * (gradient + MOMENTUM_RATE * moment)
        moment_new[at] = moment
        slow_new[at] = slow
        fast_new[at] = slow.astype(fast_new.dtype)

    def run(steps):
        seen = set()
        sent = 0
        last = max(i for i, step in enumerate(steps) if step[2] or step[3] > 2)
        ready = []
        for index, (chunk, waits, sends, kind) in enumerate(steps):
            if kind == 4:
                norms[mine] = square[:, : cols // 2] + square[:, cols // 2 :]
                for k in range(1, m):
                    norm_copy(k).start()
                continue
            if kind == 5:
                for k in range(1, m):
                    norm_copy(k).wait_recv()
                total = norms[0]
                for j in range(1, m):
                    total = total + norms[j]
                parts[me] = total
                for k in range(1, n):
                    part_copy(k).start()
                continue
            g = chunk // 4
            if kind != 2 and g not in seen:
                seen.add(g)
                for copy in load(g):
                    copy.wait()
            at = at_of(chunk)
            for k in range(3):
                if waits >> k & 1:
                    sum_copy(chunk, k).wait_recv()
            if waits & 8:
                mean_copy(chunk, 2).wait_recv()
            if kind in (0, 1, 3):
                value = part[at] if kind == 3 else slow_ref[at] - fast_ref[at].astype(jnp.float32)
                for k in range(3):
                    if waits >> k & 1:
                        value = value + inbox[k, at]
                if kind == 0:
                    part[at] = value
                else:
                    value = value * (1.0 / n)
                    pseudo[at] = value
            for k in (1, 0, 2):
                if sends >> k & 1:
                    sum_copy(chunk, k).start()
                    sent += sizes[g]
                if sends >> (3 + k) & 1:
                    mean_copy(chunk, k).start()
                    sent += sizes[g]
            if kind in (1, 3):
                weight = 1.0 if kind == 1 else 0.5
                square[...] += weight * jnp.sum((value * value).reshape(sizes[g] // 8, 8, cols), axis=0)
            if waits & 8 or kind in (1, 3):
                ready.append(chunk)
            if index == last:
                factor = clip()
                for g in loads:
                    if g not in seen:
                        for copy in load(g):
                            copy.wait()
            if index >= last:
                for other in ready:
                    update(factor, other)
                ready.clear()
        whole = inbox.reshape(3 * rows, cols).at[pl.ds(0, sent)]
        pltpu.make_async_copy(whole, whole, send_sem).wait()

    @pl.when(outer)
    def _():
        pl.semaphore_wait(barrier, m + 1)
        run(OUTER)

    @pl.when(jnp.logical_not(outer))
    def _():
        pl.semaphore_wait(barrier, m + 2)
        run(INNER)

    for k in range(1, m):
        norm_copy(k).wait_send()
    for k in range(1, n):
        part_copy(k).wait_send()


def ladder(n, m, max_norm, slow, fast, moment):
    rows, cols = slow.shape
    groups = len(SIZES)
    hbm = pl.BlockSpec(memory_space=pltpu.HBM)
    vmem = pl.BlockSpec(memory_space=pltpu.VMEM)
    whole = jax.ShapeDtypeStruct((rows, cols), jnp.float32)
    dma = pltpu.SemaphoreType.DMA
    flat = [pltpu.with_memory_space_constraint(x, pltpu.HBM) for x in (slow, fast, moment)]
    results = pl.pallas_call(
        functools.partial(ladder_kernel, n, m, max_norm),
        out_shape=(whole, whole, jax.ShapeDtypeStruct((rows, cols), fast.dtype)),
        in_specs=[hbm, hbm, hbm],
        out_specs=(vmem, vmem, vmem),
        scratch_shapes=[
            pltpu.VMEM((rows, cols), jnp.float32),
            pltpu.VMEM((rows, cols), jnp.float32),
            pltpu.VMEM((rows, cols), jnp.float32),
            pltpu.VMEM((rows, cols), fast.dtype),
            pltpu.VMEM((rows, cols), jnp.float32),
            pltpu.VMEM((3, rows, cols), jnp.float32),
            pltpu.VMEM((8, cols), jnp.float32),
            pltpu.VMEM((m, 8, cols // 2), jnp.float32),
            pltpu.VMEM((n, 8, cols // 2), jnp.float32),
            dma,
            dma((2, groups)),
            dma,
            dma((4, 4 * groups)),
            dma((m,)),
            dma((m,)),
            dma((n,)),
            dma((n,)),
        ],
        compiler_params=pltpu.CompilerParams(
            collective_id=0, has_side_effects=True, vmem_limit_bytes=LADDER_LIMIT
        ),
        name="ladder",
    )(*flat)
    return emit(results, 4)


def device_at(place, n):
    half = n // 2
    up = 2 * place
    down = 2 * (n - 1 - place) + 1
    return jnp.where(place < half, up, down)


def ring_kernel(n, m, subs, max_norm, slow_hbm, fast_hbm, moment_hbm,
           slow_out, moment_out, fast_out,
           ring, slow_ref, fast_ref, moment_ref, pseudo_ref, parts, norms, moment_sem, load_sem, send_sem, recv_sem,
           part_send, part_recv, norm_send, norm_recv):
    rows, cols = slow_ref.shape
    chunk = rows // n
    sub = chunk // subs
    half = cols // 2
    me = lax.axis_index("dp")
    mine = lax.axis_index("mp")
    z, y = me // 2, lax.rem(me, 2)
    place = jnp.where(y == 0, z, n - 1 - z)
    right = device_at(lax.rem(place + 1, n), n)
    left = device_at(lax.rem(place + n - 1, n), n)
    goal = (right, left)
    order = (place, lax.rem(n - place, n))

    def load(d, k):
        c = lax.rem(order[d] - k + n, n)
        at = (pl.ds(pl.multiple_of(c * chunk, chunk), chunk), pl.ds(d * half, half))
        return (
            pltpu.make_async_copy(slow_hbm.at[at], slow_ref.at[at], load_sem.at[0, d, k]),
            pltpu.make_async_copy(fast_hbm.at[at], fast_ref.at[at], load_sem.at[1, d, k]),
        )

    for d in range(2):
        for copy in load(d, 0):
            copy.start()
    barrier = pltpu.get_barrier_semaphore()
    for other in (left, right):
        pl.semaphore_signal(barrier, inc=1, device_id={"dp": other}, device_id_type=MESH)
    for k in range(1, m):
        pl.semaphore_signal(
            barrier, inc=1, device_id={"mp": lax.rem(mine + k, m)}, device_id_type=MESH
        )
    moment_load = pltpu.make_async_copy(moment_hbm, moment_ref, moment_sem)

    def start_row(c, b):
        return pl.multiple_of(c * chunk + b * sub, sub)

    def own(d, b, c):
        at = (pl.ds(start_row(c, b), sub), pl.ds(d * half, half))
        return slow_ref[at] - fast_ref[at].astype(jnp.float32)

    def reduce_copy(d, b, s):
        return pltpu.make_async_remote_copy(
            src_ref=ring.at[d, b, s], dst_ref=ring.at[d, b, s + 1],
            send_sem=send_sem.at[d, b, s], recv_sem=recv_sem.at[d, b, s],
            device_id={"dp": goal[d]}, device_id_type=MESH,
        )

    def gather_copy(d, b, s, c):
        at = (pl.ds(start_row(c, b), sub), pl.ds(d * half, half))
        return pltpu.make_async_remote_copy(
            src_ref=pseudo_ref.at[at], dst_ref=pseudo_ref.at[at],
            send_sem=send_sem.at[d, b, n - 1 + s], recv_sem=recv_sem.at[d, b, n - 1 + s],
            device_id={"dp": goal[d]}, device_id_type=MESH,
        )

    def part_copy(k):
        return pltpu.make_async_remote_copy(
            src_ref=parts.at[me], dst_ref=parts.at[me],
            send_sem=part_send.at[k], recv_sem=part_recv.at[k],
            device_id={"dp": lax.rem(me + k, n)}, device_id_type=MESH,
        )

    def norm_copy(k):
        return pltpu.make_async_remote_copy(
            src_ref=norms.at[mine], dst_ref=norms.at[mine],
            send_sem=norm_send.at[k], recv_sem=norm_recv.at[k],
            device_id={"mp": lax.rem(mine + k, m)}, device_id_type=MESH,
        )

    streams = [(d, b) for b in range(subs) for d in range(2)]
    for k in range(1, n):
        for d in range(2):
            for copy in load(d, k):
                copy.start()
    for d in range(2):
        for copy in load(d, 0):
            copy.wait()
    pl.semaphore_wait(barrier, 2 + m - 1)
    for d, b in streams:
        ring[d, b, 0] = own(d, b, order[d])
        reduce_copy(d, b, 0).start()
    moment_load.start()

    def reduce_step(s, carry):
        for d in range(2):
            for copy in load(d, s + 1):
                copy.wait()
        for d, b in streams:
            c = lax.rem(order[d] - s - 1 + n, n)
            reduce_copy(d, b, s).wait_recv()
            ring[d, b, s + 1] = ring[d, b, s + 1] + own(d, b, c)
            reduce_copy(d, b, s + 1).start()
        return carry

    lax.fori_loop(0, n - 2, reduce_step, 0)
    for d in range(2):
        for copy in load(d, n - 1):
            copy.wait()
    part = jnp.zeros((8, half), jnp.float32)
    for d, b in streams:
        c = lax.rem(order[d] + 1, n)
        reduce_copy(d, b, n - 2).wait_recv()
        value = (ring[d, b, n - 1] + own(d, b, c)) / n
        pseudo_ref[pl.ds(start_row(c, b), sub), pl.ds(d * half, half)] = value
        gather_copy(d, b, 0, c).start()
        part = part + jnp.sum((value * value).reshape(sub // 8, 8, half), axis=0)
    parts[me] = part

    def gather_step(s, carry):
        for d, b in streams:
            c = lax.rem(order[d] - s + n, n)
            gather_copy(d, b, s, c).wait_recv()
            gather_copy(d, b, s + 1, c).start()
        return carry

    second = (n - 2) // 2
    first = second // 2
    for k in range(1, n):
        part_copy(k).start()
    lax.fori_loop(0, first, gather_step, 0)
    for k in range(1, n):
        part_copy(k).wait_recv()
    norm = parts[0]
    for j in range(1, n):
        norm = norm + parts[j]
    norms[mine] = norm
    for k in range(1, m):
        norm_copy(k).start()
    lax.fori_loop(first, second, gather_step, 0)
    for k in range(1, m):
        norm_copy(k).wait_recv()
    total = norms[0]
    for j in range(1, m):
        total = total + norms[j]
    total = jnp.sum(jnp.sum(total, axis=1, keepdims=True), axis=0, keepdims=True)
    factor = jnp.minimum(1.0, max_norm / (jnp.sqrt(total) + EPSILON))
    moment_load.wait()

    def update(d, c, start=0, size=chunk):
        at = (pl.ds(pl.multiple_of(c * chunk + start, 16), size), pl.ds(d * half, half))
        gradient = factor * pseudo_ref[at]
        moment = MOMENTUM_RATE * moment_ref[at] + gradient
        slow = slow_ref[at] - OUTER_RATE * (gradient + MOMENTUM_RATE * moment)
        moment_out[at] = moment
        slow_out[at] = slow
        fast_out[at] = slow.astype(fast_out.dtype)

    def update_step(s, carry):
        gather_step(s, carry)
        for d in range(2):
            update(d, lax.rem(order[d] - s + n, n))
            update(d, lax.rem(order[d] - (s - second) + n, n))
        return carry

    lax.fori_loop(second, n - 2, update_step, 0)
    for d in range(2):
        update(d, lax.rem(order[d] + 1, n))
    for k in range(1, n):
        part_copy(k).wait_send()
    for k in range(1, m):
        norm_copy(k).wait_send()

    def drain(s, carry):
        for d, b in streams:
            reduce_copy(d, b, s).wait_send()
            gather_copy(d, b, s, 0).wait_send()
        return carry

    lax.fori_loop(0, n - 2, drain, 0)
    for d, b in streams:
        c = lax.rem(order[d] + 2, n)
        reduce_copy(d, b, n - 2).wait_send()
        gather_copy(d, b, n - 2, c).wait()
        update(d, c, b * sub, sub)


def emit_kernel(pieces, *refs):
    count = len(refs) // 2
    sources, targets, sem = refs[:count], refs[count:-1], refs[-1]
    size = sources[0].shape[0] // pieces
    copies = [
        pltpu.make_async_copy(
            sources[i].at[pl.ds(k * size, size)], targets[i].at[pl.ds(k * size, size)], sem.at[i, k]
        )
        for k in range(pieces) for i in range(count)
    ]
    for copy in copies:
        copy.start()
    for copy in copies:
        copy.wait()


def emit(arrays, pieces):
    return pl.pallas_call(
        functools.partial(emit_kernel, pieces),
        out_shape=tuple(jax.ShapeDtypeStruct(x.shape, x.dtype) for x in arrays),
        in_specs=[pl.BlockSpec(memory_space=pltpu.VMEM)] * len(arrays),
        out_specs=tuple(pl.BlockSpec(memory_space=pltpu.HBM) for _ in arrays),
        scratch_shapes=[pltpu.SemaphoreType.DMA((len(arrays), pieces))],
        compiler_params=pltpu.CompilerParams(vmem_limit_bytes=VMEM_LIMIT),
        name="emit",
    )(*arrays)


def ring(n, m, max_norm, slow, fast, moment):
    rows, cols = slow.shape
    subs = SUBS
    while rows % (n * subs * 16):
        subs -= 1
    sub = rows // (n * subs)
    hbm = pl.BlockSpec(memory_space=pltpu.HBM)
    vmem = pl.BlockSpec(memory_space=pltpu.VMEM)
    flat = [pltpu.with_memory_space_constraint(x, pltpu.HBM) for x in (slow, fast, moment)]
    results = pl.pallas_call(
        functools.partial(ring_kernel, n, m, subs, max_norm),
        out_shape=(
            jax.ShapeDtypeStruct((rows, cols), jnp.float32),
            jax.ShapeDtypeStruct((rows, cols), jnp.float32),
            jax.ShapeDtypeStruct((rows, cols), jnp.bfloat16),
        ),
        in_specs=[hbm, hbm, hbm],
        out_specs=(vmem, vmem, vmem),
        scratch_shapes=[
            pltpu.VMEM((2, subs, n, sub, cols // 2), jnp.float32),
            pltpu.VMEM((rows, cols), jnp.float32),
            pltpu.VMEM((rows, cols), jnp.bfloat16),
            pltpu.VMEM((rows, cols), jnp.float32),
            pltpu.VMEM((rows, cols), jnp.float32),
            pltpu.VMEM((n, 8, cols // 2), jnp.float32),
            pltpu.VMEM((m, 8, cols // 2), jnp.float32),
            pltpu.SemaphoreType.DMA,
            pltpu.SemaphoreType.DMA((2, 2, n)),
            pltpu.SemaphoreType.DMA((2, subs, 2 * n - 2)),
            pltpu.SemaphoreType.DMA((2, subs, 2 * n - 2)),
            pltpu.SemaphoreType.DMA((n,)),
            pltpu.SemaphoreType.DMA((n,)),
            pltpu.SemaphoreType.DMA((m,)),
            pltpu.SemaphoreType.DMA((m,)),
        ],
        compiler_params=pltpu.CompilerParams(
            collective_id=0, has_side_effects=True, vmem_limit_bytes=VMEM_LIMIT
        ),
        name="ring",
    )(*flat)
    return emit(results, 4)


def body(slow_weights, fast_weights, momentum):
    n, m = lax.axis_size("dp"), lax.axis_size("mp")
    layers, depth, cols = slow_weights.shape
    rows = layers * depth
    max_norm = CLIP_LEVEL * math.sqrt(rows * cols * m)
    flat = [x.reshape(rows, cols) for x in (slow_weights, fast_weights, momentum)]
    columns = n // 2
    form = ladder if columns == 4 and rows % (sum(SIZES) * 4 * 16) == 0 else ring
    slow_next, momentum_next, fast_next = form(n, m, max_norm, *flat)
    return (
        slow_next.reshape(slow_weights.shape),
        momentum_next.reshape(slow_weights.shape),
        fast_next.reshape(fast_weights.shape),
    )


def solution(mesh):
    in_specs = (P(None, None, "mp"), P("dp", None, None, "mp"), P(None, None, "mp"))
    out_specs = (P(None, None, "mp"), P(None, None, "mp"), P("dp", None, None, "mp"))
    return jax.shard_map(body, mesh=mesh, in_specs=in_specs, out_specs=out_specs, check_vma=False)
```

```python
import functools
import math

import jax
import jax.numpy as jnp
from jax import lax
from jax.experimental import pallas as pl
from jax.experimental.pallas import tpu as pltpu
from jax.sharding import PartitionSpec as P

MOMENTUM_RATE = 0.9
OUTER_RATE = 0.7
CLIP_LEVEL = 0.2
EPSILON = 1e-06
MESH = pl.DeviceIdType.MESH
SUBS = 4
VMEM_LIMIT = 24 * 1024 * 1024
LADDER_LIMIT = 40 * 1024 * 1024

SIZES = (7, 3, 5, 7, 6, 7, 6, 8, 7)
OUTER = (
    (3, 0, 4, 0), (15, 0, 1, 0), (7, 0, 1, 0), (11, 0, 4, 0), (14, 0, 1, 0), (1, 0, 4, 0),
    (6, 0, 1, 0), (19, 0, 4, 0), (2, 4, 1, 0), (9, 0, 4, 0), (10, 4, 1, 0), (17, 0, 4, 0),
    (0, 4, 1, 0), (31, 0, 4, 0), (18, 4, 1, 0), (35, 1, 4, 0), (29, 0, 1, 0), (13, 1, 4, 0),
    (16, 4, 1, 0), (5, 1, 4, 0), (30, 4, 1, 0), (27, 1, 4, 0), (33, 1, 4, 0), (23, 0, 1, 0),
    (21, 0, 4, 0), (4, 5, 8, 1), (34, 4, 1, 0), (25, 1, 4, 0), (22, 0, 1, 0), (12, 5, 40, 1),
    (16, 8, 32, 2), (26, 4, 1, 0), (8, 5, 40, 1), (18, 8, 32, 2), (24, 4, 1, 0), (28, 1, 40, 1),
    (6, 8, 32, 2), (32, 5, 40, 1), (20, 5, 40, 1), (-1, 0, 0, 4), (14, 8, 32, 2), (-1, 0, 0, 5),
    (24, 8, 32, 2), (21, 8, 8, 2), (10, 8, 32, 2), (15, 8, 8, 2), (26, 8, 32, 2), (30, 8, 32, 2),
    (11, 8, 8, 2), (34, 8, 32, 2), (0, 8, 0, 2), (2, 8, 0, 2), (1, 8, 0, 2), (3, 8, 0, 2),
    (13, 8, 0, 2), (17, 8, 0, 2), (9, 8, 0, 2), (5, 8, 0, 2), (19, 8, 0, 2), (29, 8, 0, 2),
    (7, 8, 0, 2), (33, 8, 0, 2), (25, 8, 0, 2), (27, 8, 0, 2), (22, 8, 0, 2), (31, 8, 0, 2),
    (35, 8, 0, 2), (23, 8, 0, 2),
)
INNER = (
    (3, 0, 4, 0), (1, 0, 4, 0), (35, 0, 1, 0), (33, 0, 1, 0), (11, 0, 4, 0), (27, 0, 1, 0),
    (19, 0, 4, 0), (15, 1, 2, 0), (25, 0, 1, 0), (7, 1, 2, 0), (9, 0, 4, 0), (17, 0, 4, 0),
    (14, 1, 2, 0), (6, 1, 2, 0), (13, 2, 1, 0), (31, 0, 4, 0), (5, 2, 1, 0), (2, 5, 2, 0),
    (21, 0, 4, 0), (12, 2, 1, 0), (10, 5, 2, 0), (4, 2, 1, 0), (0, 7, 56, 1), (18, 5, 2, 0),
    (8, 6, 1, 0), (29, 1, 4, 0), (2, 8, 8, 2), (1, 8, 24, 2), (16, 7, 56, 1), (30, 5, 2, 0),
    (3, 8, 8, 2), (23, 1, 4, 0), (18, 8, 40, 2), (4, 8, 48, 2), (34, 1, 2, 0), (28, 6, 1, 0),
    (6, 8, 40, 2), (22, 5, 2, 0), (5, 8, 8, 2), (32, 2, 1, 0), (12, 8, 48, 2), (26, 1, 2, 0),
    (20, 6, 1, 0), (8, 8, 48, 2), (14, 8, 8, 2), (24, 3, 56, 1), (-1, 0, 0, 4), (10, 8, 8, 2),
    (28, 8, 48, 2), (-1, 0, 0, 5), (26, 8, 40, 2), (32, 8, 48, 2), (20, 8, 16, 2), (30, 8, 40, 2),
    (34, 8, 40, 2), (21, 8, 16, 2), (22, 8, 8, 2), (23, 8, 8, 2), (17, 8, 0, 2), (19, 8, 0, 2),
    (7, 8, 0, 2), (13, 8, 0, 2), (9, 8, 0, 2), (25, 8, 0, 2), (29, 8, 0, 2), (27, 8, 0, 2),
    (33, 8, 0, 2), (15, 8, 0, 2), (31, 8, 0, 2), (11, 8, 0, 2), (35, 8, 0, 2),
)

def ladder_kernel(n, m, max_norm, slow_hbm, fast_hbm, moment_hbm,
                  slow_new, moment_new, fast_new,
                  pseudo, slow_ref, moment_ref, fast_ref, part, inbox, square, norms, parts,
                  moment_sem, load_sem, send_sem, recv_sem, norm_send, norm_recv, part_send, part_recv):
    rows, cols = slow_ref.shape
    groups = load_sem.shape[1]
    unit = rows // (4 * sum(SIZES))
    sizes = [unit * s for s in SIZES]
    bases = [4 * sum(sizes[:g]) for g in range(groups)]
    half = n // 4
    me = lax.axis_index("dp")
    mine = lax.axis_index("mp")
    z, y = me // 2, lax.rem(me, 2)
    upper = z // half
    step = 1 - 2 * upper
    outer = lax.rem(z + upper, half) == 0
    away = jnp.where(outer, step, -step)
    near = 2 * (z + away) + y
    across = 2 * (z + step) + y
    rung = 2 * z + 1 - y
    target = (near, across, rung)
    spots = [(far + upper - 2 * far * upper) * 2 + (other + y - 2 * other * y) for far in range(2) for other in range(2)]

    def load(g):
        at = pl.ds(bases[g], 4 * sizes[g])
        return (
            pltpu.make_async_copy(slow_hbm.at[at], slow_ref.at[at], load_sem.at[0, g]),
            pltpu.make_async_copy(fast_hbm.at[at], fast_ref.at[at], load_sem.at[1, g]),
        )

    loads = []
    for entry in OUTER + INNER:
        if entry[0] >= 0 and entry[0] // 4 not in loads:
            loads.append(entry[0] // 4)
    for g in loads[:2]:
        for copy in load(g):
            copy.start()
    barrier = pltpu.get_barrier_semaphore()
    for other in (near, rung):
        pl.semaphore_signal(barrier, inc=1, device_id={"dp": other}, device_id_type=MESH)
    for k in range(1, m):
        pl.semaphore_signal(
            barrier, inc=1, device_id={"mp": lax.rem(mine + k, m)}, device_id_type=MESH
        )

    @pl.when(jnp.logical_not(outer))
    def _():
        pl.semaphore_signal(barrier, inc=1, device_id={"dp": across}, device_id_type=MESH)

    for g in loads[2:]:
        for copy in load(g):
            copy.start()
    moment_load = pltpu.make_async_copy(moment_hbm, moment_ref, moment_sem)
    moment_load.start()
    square[...] = jnp.zeros_like(square)

    def at_of(chunk):
        g = chunk // 4
        return pl.ds(pl.multiple_of(bases[g] + spots[chunk % 4] * sizes[g], 16), sizes[g])

    def sum_copy(chunk, k):
        at = at_of(chunk)
        return pltpu.make_async_remote_copy(
            src_ref=part.at[at], dst_ref=inbox.at[k, at], send_sem=send_sem,
            recv_sem=recv_sem.at[k, chunk // 4 * 4 + spots[chunk % 4]],
            device_id={"dp": target[k]}, device_id_type=MESH,
        )

    def mean_copy(chunk, k):
        at = at_of(chunk)
        return pltpu.make_async_remote_copy(
            src_ref=pseudo.at[at], dst_ref=pseudo.at[at], send_sem=send_sem,
            recv_sem=recv_sem.at[3, chunk // 4 * 4 + spots[chunk % 4]],
            device_id={"dp": target[k]}, device_id_type=MESH,
        )

    def norm_copy(k):
        return pltpu.make_async_remote_copy(
            src_ref=norms.at[mine], dst_ref=norms.at[mine], send_sem=norm_send.at[k], recv_sem=norm_recv.at[k],
            device_id={"mp": lax.rem(mine + k, m)}, device_id_type=MESH,
        )

    def part_copy(k):
        return pltpu.make_async_remote_copy(
            src_ref=parts.at[me], dst_ref=parts.at[me], send_sem=part_send.at[k], recv_sem=part_recv.at[k],
            device_id={"dp": lax.rem(me + k, n)}, device_id_type=MESH,
        )

    def clip():
        for k in range(1, n):
            part_copy(k).wait_recv()
        total = parts[0]
        for j in range(1, n):
            total = total + parts[j]
        total = jnp.sum(jnp.sum(total, axis=1, keepdims=True), axis=0, keepdims=True)
        moment_load.wait()
        return jnp.minimum(1.0, max_norm / (jnp.sqrt(total) + EPSILON))

    def update(factor, chunk):
        at = at_of(chunk)
        gradient = factor * pseudo[at]
        moment = MOMENTUM_RATE * moment_ref[at] + gradient
        slow = slow_ref[at] - OUTER_RATE * (gradient + MOMENTUM_RATE * moment)
        moment_new[at] = moment
        slow_new[at] = slow
        fast_new[at] = slow.astype(fast_new.dtype)

    def run(steps):
        seen = set()
        sent = 0
        last = max(i for i, step in enumerate(steps) if step[2] or step[3] > 2)
        ready = []
        for index, (chunk, waits, sends, kind) in enumerate(steps):
            if kind == 4:
                norms[mine] = square[:, : cols // 2] + square[:, cols // 2 :]
                for k in range(1, m):
                    norm_copy(k).start()
                continue
            if kind == 5:
                for k in range(1, m):
                    norm_copy(k).wait_recv()
                total = norms[0]
                for j in range(1, m):
                    total = total + norms[j]
                parts[me] = total
                for k in range(1, n):
                    part_copy(k).start()
                continue
            g = chunk // 4
            if kind != 2 and g not in seen:
                seen.add(g)
                for copy in load(g):
                    copy.wait()
            at = at_of(chunk)
            for k in range(3):
                if waits >> k & 1:
                    sum_copy(chunk, k).wait_recv()
            if waits & 8:
                mean_copy(chunk, 2).wait_recv()
            if kind in (0, 1, 3):
                value = part[at] if kind == 3 else slow_ref[at] - fast_ref[at].astype(jnp.float32)
                for k in range(3):
                    if waits >> k & 1:
                        value = value + inbox[k, at]
                if kind == 0:
                    part[at] = value
                else:
                    value = value * (1.0 / n)
                    pseudo[at] = value
            for k in (1, 0, 2):
                if sends >> k & 1:
                    sum_copy(chunk, k).start()
                    sent += sizes[g]
                if sends >> (3 + k) & 1:
                    mean_copy(chunk, k).start()
                    sent += sizes[g]
            if kind in (1, 3):
                weight = 1.0 if kind == 1 else 0.5
                square[...] += weight * jnp.sum((value * value).reshape(sizes[g] // 8, 8, cols), axis=0)
            if waits & 8 or kind in (1, 3):
                ready.append(chunk)
            if index == last:
                factor = clip()
                for g in loads:
                    if g not in seen:
                        for copy in load(g):
                            copy.wait()
            if index >= last:
                for other in ready:
                    update(factor, other)
                ready.clear()
        whole = inbox.reshape(3 * rows, cols).at[pl.ds(0, sent)]
        pltpu.make_async_copy(whole, whole, send_sem).wait()

    @pl.when(outer)
    def _():
        pl.semaphore_wait(barrier, m + 1)
        run(OUTER)

    @pl.when(jnp.logical_not(outer))
    def _():
        pl.semaphore_wait(barrier, m + 2)
        run(INNER)

    for k in range(1, m):
        norm_copy(k).wait_send()
    for k in range(1, n):
        part_copy(k).wait_send()


def ladder(n, m, max_norm, slow, fast, moment):
    rows, cols = slow.shape
    groups = len(SIZES)
    hbm = pl.BlockSpec(memory_space=pltpu.HBM)
    vmem = pl.BlockSpec(memory_space=pltpu.VMEM)
    whole = jax.ShapeDtypeStruct((rows, cols), jnp.float32)
    dma = pltpu.SemaphoreType.DMA
    flat = [pltpu.with_memory_space_constraint(x, pltpu.HBM) for x in (slow, fast, moment)]
    results = pl.pallas_call(
        functools.partial(ladder_kernel, n, m, max_norm),
        out_shape=(whole, whole, jax.ShapeDtypeStruct((rows, cols), fast.dtype)),
        in_specs=[hbm, hbm, hbm],
        out_specs=(vmem, vmem, vmem),
        scratch_shapes=[
            pltpu.VMEM((rows, cols), jnp.float32),
            pltpu.VMEM((rows, cols), jnp.float32),
            pltpu.VMEM((rows, cols), jnp.float32),
            pltpu.VMEM((rows, cols), fast.dtype),
            pltpu.VMEM((rows, cols), jnp.float32),
            pltpu.VMEM((3, rows, cols), jnp.float32),
            pltpu.VMEM((8, cols), jnp.float32),
            pltpu.VMEM((m, 8, cols // 2), jnp.float32),
            pltpu.VMEM((n, 8, cols // 2), jnp.float32),
            dma,
            dma((2, groups)),
            dma,
            dma((4, 4 * groups)),
            dma((m,)),
            dma((m,)),
            dma((n,)),
            dma((n,)),
        ],
        compiler_params=pltpu.CompilerParams(
            collective_id=0, has_side_effects=True, vmem_limit_bytes=LADDER_LIMIT
        ),
        name="ladder",
    )(*flat)
    return emit(results, 4)


def device_at(place, n):
    half = n // 2
    up = 2 * place
    down = 2 * (n - 1 - place) + 1
    return jnp.where(place < half, up, down)


def ring_kernel(n, m, subs, max_norm, slow_hbm, fast_hbm, moment_hbm,
           slow_out, moment_out, fast_out,
           ring, slow_ref, fast_ref, moment_ref, pseudo_ref, parts, norms, moment_sem, load_sem, send_sem, recv_sem,
           part_send, part_recv, norm_send, norm_recv):
    rows, cols = slow_ref.shape
    chunk = rows // n
    sub = chunk // subs
    half = cols // 2
    me = lax.axis_index("dp")
    mine = lax.axis_index("mp")
    z, y = me // 2, lax.rem(me, 2)
    place = jnp.where(y == 0, z, n - 1 - z)
    right = device_at(lax.rem(place + 1, n), n)
    left = device_at(lax.rem(place + n - 1, n), n)
    goal = (right, left)
    order = (place, lax.rem(n - place, n))

    def load(d, k):
        c = lax.rem(order[d] - k + n, n)
        at = (pl.ds(pl.multiple_of(c * chunk, chunk), chunk), pl.ds(d * half, half))
        return (
            pltpu.make_async_copy(slow_hbm.at[at], slow_ref.at[at], load_sem.at[0, d, k]),
            pltpu.make_async_copy(fast_hbm.at[at], fast_ref.at[at], load_sem.at[1, d, k]),
        )

    for d in range(2):
        for copy in load(d, 0):
            copy.start()
    barrier = pltpu.get_barrier_semaphore()
    for other in (left, right):
        pl.semaphore_signal(barrier, inc=1, device_id={"dp": other}, device_id_type=MESH)
    for k in range(1, m):
        pl.semaphore_signal(
            barrier, inc=1, device_id={"mp": lax.rem(mine + k, m)}, device_id_type=MESH
        )
    moment_load = pltpu.make_async_copy(moment_hbm, moment_ref, moment_sem)

    def start_row(c, b):
        return pl.multiple_of(c * chunk + b * sub, sub)

    def own(d, b, c):
        at = (pl.ds(start_row(c, b), sub), pl.ds(d * half, half))
        return slow_ref[at] - fast_ref[at].astype(jnp.float32)

    def reduce_copy(d, b, s):
        return pltpu.make_async_remote_copy(
            src_ref=ring.at[d, b, s], dst_ref=ring.at[d, b, s + 1],
            send_sem=send_sem.at[d, b, s], recv_sem=recv_sem.at[d, b, s],
            device_id={"dp": goal[d]}, device_id_type=MESH,
        )

    def gather_copy(d, b, s, c):
        at = (pl.ds(start_row(c, b), sub), pl.ds(d * half, half))
        return pltpu.make_async_remote_copy(
            src_ref=pseudo_ref.at[at], dst_ref=pseudo_ref.at[at],
            send_sem=send_sem.at[d, b, n - 1 + s], recv_sem=recv_sem.at[d, b, n - 1 + s],
            device_id={"dp": goal[d]}, device_id_type=MESH,
        )

    def part_copy(k):
        return pltpu.make_async_remote_copy(
            src_ref=parts.at[me], dst_ref=parts.at[me],
            send_sem=part_send.at[k], recv_sem=part_recv.at[k],
            device_id={"dp": lax.rem(me + k, n)}, device_id_type=MESH,
        )

    def norm_copy(k):
        return pltpu.make_async_remote_copy(
            src_ref=norms.at[mine], dst_ref=norms.at[mine],
            send_sem=norm_send.at[k], recv_sem=norm_recv.at[k],
            device_id={"mp": lax.rem(mine + k, m)}, device_id_type=MESH,
        )

    streams = [(d, b) for b in range(subs) for d in range(2)]
    for k in range(1, n):
        for d in range(2):
            for copy in load(d, k):
                copy.start()
    for d in range(2):
        for copy in load(d, 0):
            copy.wait()
    pl.semaphore_wait(barrier, 2 + m - 1)
    for d, b in streams:
        ring[d, b, 0] = own(d, b, order[d])
        reduce_copy(d, b, 0).start()
    moment_load.start()

    def reduce_step(s, carry):
        for d in range(2):
            for copy in load(d, s + 1):
                copy.wait()
        for d, b in streams:
            c = lax.rem(order[d] - s - 1 + n, n)
            reduce_copy(d, b, s).wait_recv()
            ring[d, b, s + 1] = ring[d, b, s + 1] + own(d, b, c)
            reduce_copy(d, b, s + 1).start()
        return carry

    lax.fori_loop(0, n - 2, reduce_step, 0)
    for d in range(2):
        for copy in load(d, n - 1):
            copy.wait()
    part = jnp.zeros((8, half), jnp.float32)
    for d, b in streams:
        c = lax.rem(order[d] + 1, n)
        reduce_copy(d, b, n - 2).wait_recv()
        value = (ring[d, b, n - 1] + own(d, b, c)) / n
        pseudo_ref[pl.ds(start_row(c, b), sub), pl.ds(d * half, half)] = value
        gather_copy(d, b, 0, c).start()
        part = part + jnp.sum((value * value).reshape(sub // 8, 8, half), axis=0)
    parts[me] = part

    def gather_step(s, carry):
        for d, b in streams:
            c = lax.rem(order[d] - s + n, n)
            gather_copy(d, b, s, c).wait_recv()
            gather_copy(d, b, s + 1, c).start()
        return carry

    second = (n - 2) // 2
    first = second // 2
    for k in range(1, n):
        part_copy(k).start()
    lax.fori_loop(0, first, gather_step, 0)
    for k in range(1, n):
        part_copy(k).wait_recv()
    norm = parts[0]
    for j in range(1, n):
        norm = norm + parts[j]
    norms[mine] = norm
    for k in range(1, m):
        norm_copy(k).start()
    lax.fori_loop(first, second, gather_step, 0)
    for k in range(1, m):
        norm_copy(k).wait_recv()
    total = norms[0]
    for j in range(1, m):
        total = total + norms[j]
    total = jnp.sum(jnp.sum(total, axis=1, keepdims=True), axis=0, keepdims=True)
    factor = jnp.minimum(1.0, max_norm / (jnp.sqrt(total) + EPSILON))
    moment_load.wait()

    def update(d, c, start=0, size=chunk):
        at = (pl.ds(pl.multiple_of(c * chunk + start, 16), size), pl.ds(d * half, half))
        gradient = factor * pseudo_ref[at]
        moment = MOMENTUM_RATE * moment_ref[at] + gradient
        slow = slow_ref[at] - OUTER_RATE * (gradient + MOMENTUM_RATE * moment)
        moment_out[at] = moment
        slow_out[at] = slow
        fast_out[at] = slow.astype(fast_out.dtype)

    def update_step(s, carry):
        gather_step(s, carry)
        for d in range(2):
            update(d, lax.rem(order[d] - s + n, n))
            update(d, lax.rem(order[d] - (s - second) + n, n))
        return carry

    lax.fori_loop(second, n - 2, update_step, 0)
    for d in range(2):
        update(d, lax.rem(order[d] + 1, n))
    for k in range(1, n):
        part_copy(k).wait_send()
    for k in range(1, m):
        norm_copy(k).wait_send()

    def drain(s, carry):
        for d, b in streams:
            reduce_copy(d, b, s).wait_send()
            gather_copy(d, b, s, 0).wait_send()
        return carry

    lax.fori_loop(0, n - 2, drain, 0)
    for d, b in streams:
        c = lax.rem(order[d] + 2, n)
        reduce_copy(d, b, n - 2).wait_send()
        gather_copy(d, b, n - 2, c).wait()
        update(d, c, b * sub, sub)


def emit_kernel(pieces, *refs):
    count = len(refs) // 2
    sources, targets, sem = refs[:count], refs[count:-1], refs[-1]
    size = sources[0].shape[0] // pieces
    copies = [
        pltpu.make_async_copy(
            sources[i].at[pl.ds(k * size, size)], targets[i].at[pl.ds(k * size, size)], sem.at[i, k]
        )
        for k in range(pieces) for i in range(count)
    ]
    for copy in copies:
        copy.start()
    for copy in copies:
        copy.wait()


def emit(arrays, pieces):
    return pl.pallas_call(
        functools.partial(emit_kernel, pieces),
        out_shape=tuple(jax.ShapeDtypeStruct(x.shape, x.dtype) for x in arrays),
        in_specs=[pl.BlockSpec(memory_space=pltpu.VMEM)] * len(arrays),
        out_specs=tuple(pl.BlockSpec(memory_space=pltpu.HBM) for _ in arrays),
        scratch_shapes=[pltpu.SemaphoreType.DMA((len(arrays), pieces))],
        compiler_params=pltpu.CompilerParams(vmem_limit_bytes=VMEM_LIMIT),
        name="emit",
    )(*arrays)


def ring(n, m, max_norm, slow, fast, moment):
    rows, cols = slow.shape
    subs = SUBS
    while rows % (n * subs * 16):
        subs -= 1
    sub = rows // (n * subs)
    hbm = pl.BlockSpec(memory_space=pltpu.HBM)
    vmem = pl.BlockSpec(memory_space=pltpu.VMEM)
    flat = [pltpu.with_memory_space_constraint(x, pltpu.HBM) for x in (slow, fast, moment)]
    results = pl.pallas_call(
        functools.partial(ring_kernel, n, m, subs, max_norm),
        out_shape=(
            jax.ShapeDtypeStruct((rows, cols), jnp.float32),
            jax.ShapeDtypeStruct((rows, cols), jnp.float32),
            jax.ShapeDtypeStruct((rows, cols), jnp.bfloat16),
        ),
        in_specs=[hbm, hbm, hbm],
        out_specs=(vmem, vmem, vmem),
        scratch_shapes=[
            pltpu.VMEM((2, subs, n, sub, cols // 2), jnp.float32),
            pltpu.VMEM((rows, cols), jnp.float32),
            pltpu.VMEM((rows, cols), jnp.bfloat16),
            pltpu.VMEM((rows, cols), jnp.float32),
            pltpu.VMEM((rows, cols), jnp.float32),
            pltpu.VMEM((n, 8, cols // 2), jnp.float32),
            pltpu.VMEM((m, 8, cols // 2), jnp.float32),
            pltpu.SemaphoreType.DMA,
            pltpu.SemaphoreType.DMA((2, 2, n)),
            pltpu.SemaphoreType.DMA((2, subs, 2 * n - 2)),
            pltpu.SemaphoreType.DMA((2, subs, 2 * n - 2)),
            pltpu.SemaphoreType.DMA((n,)),
            pltpu.SemaphoreType.DMA((n,)),
            pltpu.SemaphoreType.DMA((m,)),
            pltpu.SemaphoreType.DMA((m,)),
        ],
        compiler_params=pltpu.CompilerParams(
            collective_id=0, has_side_effects=True, vmem_limit_bytes=VMEM_LIMIT
        ),
        name="ring",
    )(*flat)
    return emit(results, 4)


def body(slow_weights, fast_weights, momentum):
    n, m = lax.axis_size("dp"), lax.axis_size("mp")
    layers, depth, cols = slow_weights.shape
    rows = layers * depth
    max_norm = CLIP_LEVEL * math.sqrt(rows * cols * m)
    flat = [x.reshape(rows, cols) for x in (slow_weights, fast_weights, momentum)]
    columns = n // 2
    form = ladder if columns == 4 and rows % (sum(SIZES) * 4 * 16) == 0 else ring
    slow_next, momentum_next, fast_next = form(n, m, max_norm, *flat)
    return (
        slow_next.reshape(slow_weights.shape),
        momentum_next.reshape(slow_weights.shape),
        fast_next.reshape(fast_weights.shape),
    )


def solution(mesh):
    in_specs = (P(None, None, "mp"), P("dp", None, None, "mp"), P(None, None, "mp"))
    out_specs = (P(None, None, "mp"), P(None, None, "mp"), P("dp", None, None, "mp"))
    return jax.shard_map(body, mesh=mesh, in_specs=in_specs, out_specs=out_specs, check_vma=False)
```
